512 devices in a mesh: tm: 16 (over y_lo, x, core), rep: 32 (over y_hi, z).
Axes of the slice: x: 4, y: 4 (y_hi: 2, y_lo: 2; y = y_hi * 2 + y_lo), z: 16, core: 2. Of those that a mesh axis runs over, the one named last changes fastest.
Arguments:
- snapshots: float32 [128, 256, 1024], P('tm', 'rep'), may hold values from -6 to 6
- freq_bins: int32 [32], replicated, may hold values from 1 to 511
- replicas: float32 [2, 32, 32768, 256], P(None, 'tm', 'rep'), may hold values from -6 to 6
Outputs:
- power: float32 [32768], P(('rep', 'tm'))
The draws below stay inside these ranges and needn't reach their ends.
All inputs are finite; a program needn't handle non-finite values.
Results may differ from the reference program's by a relative error of at most 0.00005.
Values sent between devices are 32-bit elements; how exact they have to be, the bound alone decides.
A program may use at most 64 MiB of HBM per device.

```python
import math
import jax
import jax.numpy as jnp
from jax import lax

ELEMS = 256
SAMPLES = 1024
BINS = 32
SNAPS = 128
GRID = 32768


def place_ends(drawn, own_key, low, high):
    extent = drawn.shape
    index_at = [jax.random.randint(jax.random.fold_in(own_key, axis), (), 0, extent[axis]) for axis in range(len(extent))]
    drawn = drawn.at[tuple(index_at)].set(low)
    longest = extent.index(max(extent))
    index_at[longest] = (index_at[longest] + 1) % extent[longest]
    return drawn.at[tuple(index_at)].set(high)


def block_levels(rng, shape, split, smallest, high):
    def one(dim, parts):
        draws = jax.random.uniform(jax.random.fold_in(jax.random.fold_in(rng, 6), dim), (parts,), jnp.float32, smallest / len(split), high / len(split))
        return jnp.repeat(jnp.exp(draws), shape[dim] // parts).reshape((-1,) + (1,) * (len(shape) - dim - 1))

    loudness = one(*split[0])
    for cut in split[1:]:
        loudness = loudness * one(*cut)
    return loudness


def normal_values(key, dims, scale, most, shards=(), kind=jnp.bfloat16):
    factor_of = block_levels(key, dims, shards, -0.22, 0.18) if shards else 1.0
    entries = jax.random.normal(key, dims, jnp.float32) * scale * factor_of
    return jnp.minimum(jnp.maximum(entries, -most), most).astype(kind)


def setup_inputs(seed: int = 0) -> dict:
    seeds = jax.random.split(jax.random.key(seed), 4)
    snapshots = normal_values(seeds[0], (SNAPS, ELEMS, SAMPLES), 1.0, 6.0, ((0, 16), (1, 32)), jnp.float32)
    freq_bins = place_ends(jax.random.randint(seeds[1], (BINS,), 1, SAMPLES // 2), jax.random.fold_in(seeds[1], 1), 1, (SAMPLES // 2) - 1).astype(jnp.int32)
    replicas = normal_values(seeds[2], (2, BINS, GRID, ELEMS), 1.0, 6.0, ((1, 16), (2, 32)), jnp.float32)
    return dict(snapshots=snapshots, freq_bins=freq_bins, replicas=replicas)


epsilon = 1e-6


def dft_table(freq_bins, length):
    offsets = jnp.arange(length, dtype=jnp.int32)
    phases = (offsets[:, None] * freq_bins[None, :]) % length
    angles = phases.astype(jnp.float32) * (2.0 * math.pi / length)
    window = 0.5 - 0.5 * jnp.cos(offsets.astype(jnp.float32) * (2.0 * math.pi / length))
    return jnp.concatenate([window[:, None] * jnp.cos(angles), -window[:, None] * jnp.sin(angles)], axis=1)


def reference(snapshots, freq_bins, replicas):
    dft_rows = dft_table(freq_bins, SAMPLES)
    spectra = jnp.dot(snapshots.reshape(SNAPS * ELEMS, SAMPLES), dft_rows, precision=lax.Precision.HIGHEST, preferred_element_type=jnp.float32).reshape(SNAPS, ELEMS, 2, BINS)

    def one_bin(column):
        spec_re = lax.dynamic_index_in_dim(spectra[:, :, 0, :], column, 2, keepdims=False)
        spec_im = lax.dynamic_index_in_dim(spectra[:, :, 1, :], column, 2, keepdims=False)
        rep_pair = lax.dynamic_index_in_dim(replicas, column, 1, keepdims=False)
        rep_re = rep_pair[0]
        rep_im = rep_pair[1]
        power_trace = jnp.sum(spec_re * spec_re + spec_im * spec_im) / SNAPS + epsilon
        norm_sq = jnp.sum(rep_re * rep_re + rep_im * rep_im, axis=1) + epsilon
        proj_re = jnp.dot(rep_re, spec_re.T, precision=lax.Precision.HIGHEST, preferred_element_type=jnp.float32) + jnp.dot(rep_im, spec_im.T, precision=lax.Precision.HIGHEST, preferred_element_type=jnp.float32)
        proj_im = jnp.dot(rep_re, spec_im.T, precision=lax.Precision.HIGHEST, preferred_element_type=jnp.float32) - jnp.dot(rep_im, spec_re.T, precision=lax.Precision.HIGHEST, preferred_element_type=jnp.float32)
        quadratic = jnp.sum(proj_re * proj_re + proj_im * proj_im, axis=1) / SNAPS
        return quadratic / (norm_sq * power_trace / ELEMS)

    per_bin = lax.map(one_bin, jnp.arange(BINS, dtype=jnp.int32))
    return jnp.sum(per_bin, axis=0) / BINS
```

```python
import functools
import math

import jax
import jax.numpy as jnp
from jax import lax
from jax.experimental import pallas as pl
from jax.experimental.pallas import tpu as pltpu
from jax.sharding import PartitionSpec as P

EPS = 1e-6
PLANES = 16
COLUMNS = 2
STEP = 2
ROWS = 256
MESH = pl.DeviceIdType.MESH
F32 = jnp.float32
BF16 = jnp.bfloat16


def split(value):
    high = value.astype(BF16)
    low = (value - high.astype(F32)).astype(BF16)
    return high, low


def lane_iota(shape):
    return lax.broadcasted_iota(jnp.int32, shape, len(shape) - 1)


def row_sums(value):
    folded = value[:, :128] + value[:, 128:]
    return jnp.sum(folded.T, axis=0, keepdims=True)


def fused(peers, bins_ref, snaps_hbm, reps_hbm, out_ref, snaps, reps, table, pieces, landed, blocks, left, right_hi,
          right_lo, norms, quads, shares, arrived, load_sem, piece_send, piece_recv, block_send, block_recv, share_send,
          share_recv):
    me = lax.axis_index("tm")
    spot = lax.axis_index("rep")
    column = spot // PLANES
    plane = spot % PLANES
    bin_count = bins_ref.shape[0]
    snap_rows, elem_rows, samples = snaps.shape
    grid_rows = reps.shape[2]
    elems = reps.shape[3]

    def rep_at(col, z):
        return col * PLANES + lax.rem(z + 2 * PLANES, PLANES)

    up = min(STEP, PLANES // 2)
    down = min(STEP, PLANES // 2 - 1)
    near = sorted(set([d for d in range(1, up + 1)] + [-d for d in range(1, down + 1)]
                      + [-d for d in range(1, up + 1)] + [d for d in range(1, down + 1)]))

    barrier = pltpu.get_barrier_semaphore()

    def greet(off, carry):
        other = lax.rem(me + off, peers)
        pl.semaphore_signal(barrier, inc=1, device_id={"tm": other, "rep": rep_at(column, plane)}, device_id_type=MESH)
        pl.semaphore_signal(barrier, inc=1, device_id={"tm": other, "rep": rep_at(1 - column, plane)},
                            device_id_type=MESH)
        return carry

    lax.fori_loop(1, peers, greet, 0)
    pl.semaphore_signal(barrier, inc=1, device_id={"tm": me, "rep": rep_at(1 - column, plane)}, device_id_type=MESH)
    for d in near:
        pl.semaphore_signal(barrier, inc=1, device_id={"tm": me, "rep": rep_at(column, plane + d)},
                            device_id_type=MESH)
    greeted = 2 * (peers - 1) + 1 + len(near)

    snap_load = pltpu.make_async_copy(snaps_hbm, snaps, load_sem.at[0])
    snap_load.start()
    rep_loads = [pltpu.make_async_copy(reps_hbm.at[:, b], reps.at[:, b], load_sem.at[1 + b]) for b in range(2)]
    for load in rep_loads:
        load.start()

    lane = lane_iota((1, 128))
    chosen = jnp.zeros((1, 128), jnp.int32)
    for k in range(bin_count):
        chosen = jnp.where((lane & 63) // 2 == k, bins_ref[k], chosen)
    index = lax.broadcasted_iota(jnp.int32, (32, 128), 0)
    unit = 2.0 * math.pi / samples
    coarse = ((index * 32 * chosen) & (samples - 1)).astype(F32) * unit
    fine = ((index * chosen) & (samples - 1)).astype(F32) * unit
    cos_a, sin_a = jnp.cos(coarse), jnp.sin(coarse)
    cos_b, sin_b = jnp.cos(fine), jnp.sin(fine)
    real = (lane & 1) == 0
    with_cos = jnp.where(real, cos_b, -sin_b)
    with_sin = jnp.where(real, -sin_b, -cos_b)
    for a in range(samples // 32):
        rows = cos_a[a : a + 1] * with_cos + sin_a[a : a + 1] * with_sin
        high = rows.astype(BF16).astype(F32)
        table[32 * a : 32 * a + 32, :] = jnp.where(lane < 64, high, rows - high).astype(BF16)
    window = 0.5 - 0.5 * jnp.cos(lane_iota((1, samples)).astype(F32) * unit)

    quarter = me % 4
    wide = lane_iota((1, 4 * 128))
    owner = (wide // 128) * 4 + (((wide // 32) % 4 + 4 - quarter) & 3)
    key = owner * 4 + (wide // 8) % 4
    spread = (lax.broadcasted_iota(jnp.int32, (128, 512), 0) & 63 == key).astype(F32).astype(BF16)

    snap_load.wait()
    shaded = snaps[...].reshape(snap_rows * elem_rows, samples) * window
    high, low = split(shaded)
    spectra = jnp.dot(jnp.concatenate([high, low], axis=0), table[...], preferred_element_type=F32)
    high, low = split(spectra)
    placed = jnp.dot(jnp.concatenate([high, low], axis=0), spread, preferred_element_type=F32)
    slabs = jnp.sum(placed.reshape(4, snap_rows, elem_rows, 512), axis=0)
    merged = jnp.zeros((elem_rows, 512), F32)
    for s in range(snap_rows):
        merged = jnp.where((wide & 7) == s, slabs[s], merged)
    for tile in range(4):
        part = merged[:, 128 * tile : 128 * tile + 128]
        for d in range(4):
            pieces[4 * tile + d] = part if d == 0 else pltpu.roll(part, 128 - 32 * d, 1)
    landed[column, me] = pieces[me]

    pl.semaphore_wait(barrier, greeted)

    def piece_copy(other, source, col, col_from):
        return pltpu.make_async_remote_copy(
            src_ref=pieces.at[other], dst_ref=landed.at[col_from, source], send_sem=piece_send.at[col, other],
            recv_sem=piece_recv.at[col_from, source], device_id={"tm": other, "rep": rep_at(col, plane)},
            device_id_type=MESH)

    def send_pieces(off, carry):
        other = lax.rem(me + off, peers)
        piece_copy(other, me, column, column).start()
        piece_copy(other, me, 1 - column, column).start()
        return carry

    piece_copy(me, me, 1 - column, column).start()
    lax.fori_loop(1, peers, send_pieces, 0)

    for b in range(2):
        rep_loads[b].wait()

        def prepare(step, carry, b=b):
            at = pl.ds(pl.multiple_of(step * 128, 128), 128)
            re = reps[0, b, at, :]
            im = reps[1, b, at, :]
            re_hi, re_lo = split(re)
            im_hi, im_lo = split(im)
            left[b, at, 0:elems] = re_hi
            left[b, at, elems : 2 * elems] = im_hi
            left[b, at, 2 * elems : 3 * elems] = re_lo
            left[b, at, 3 * elems : 4 * elems] = im_lo
            norms[b, pl.ds(step, 1), :] = row_sums(re * re + im * im)
            return carry

        lax.fori_loop(0, grid_rows // 128, prepare, 0)

    def take_pieces(off, carry):
        other = lax.rem(me + off, peers)
        piece_copy(other, other, column, column).wait_recv()
        piece_copy(other, other, column, 1 - column).wait_recv()
        return carry

    piece_copy(me, me, column, 1 - column).wait_recv()
    lax.fori_loop(1, peers, take_pieces, 0)

    for col in range(COLUMNS):
        tiles = []
        for tile in range(4):
            got = landed[col, 4 * tile]
            for d in range(1, 4):
                got = jnp.where(lane // 32 == d, landed[col, 4 * tile + d], got)
            tiles.append(got)
        for pair in range(2):
            first, second = tiles[2 * pair], tiles[2 * pair + 1]
            blocks[plane, col, pair] = jnp.where(lane & 16 == 0, first, pltpu.roll(second, 16, 1))
            blocks[plane, col, 2 + pair] = jnp.where(lane & 16 == 0, pltpu.roll(first, 112, 1), second)

    started = []

    def block_copy(owner_plane, to, slot):
        return pltpu.make_async_remote_copy(
            src_ref=blocks.at[owner_plane], dst_ref=blocks.at[owner_plane], send_sem=block_send.at[slot],
            recv_sem=block_recv.at[owner_plane], device_id={"tm": me, "rep": rep_at(column, plane + to)},
            device_id_type=MESH)

    def plane_at(offset):
        return lax.rem(plane + offset + 2 * PLANES, PLANES)

    def pass_on(owner_plane, to):
        copy = block_copy(owner_plane, to, len(started))
        copy.start()
        started.append(copy)

    waited = set()

    def wait_block(offset):
        block_copy(plane_at(offset), 0, 0).wait_recv()
        waited.add(offset)

    top, bottom = PLANES // 2, PLANES // 2 - 1
    for reach in range(STEP, 0, -1):
        if reach <= top:
            pass_on(plane, reach)
        if reach <= bottom:
            pass_on(plane, -reach)
    hub = STEP
    while hub < top:
        wait_block(-hub)
        for reach in range(min(STEP, top - hub), 0, -1):
            pass_on(plane_at(-hub), reach)
        if hub < bottom:
            wait_block(hub)
            for reach in range(min(STEP, bottom - hub), 0, -1):
                pass_on(plane_at(hub), -reach)
        hub += STEP
    for distance in range(1, top + 1):
        for offset in (-distance, distance):
            if offset not in waited and (offset < 0 or distance <= bottom):
                wait_block(offset)

    real = (lane & 8) == 0
    traces = []
    for b in range(2):
        energy = jnp.zeros((8, 128), F32)
        for col in range(COLUMNS):
            for pair in range(2):
                value = blocks[:, col, 2 * b + pair].reshape(PLANES * elem_rows, 128)
                turned = jnp.where(real, pltpu.roll(value, 120, 1), -pltpu.roll(value, 8, 1))
                energy = energy + jnp.sum((value * value).reshape(PLANES, 8, 128), axis=0)
                for part, entry in ((0, value), (1, turned)):
                    high, low = split(entry)
                    at = part * elems + col * PLANES * elem_rows
                    right_hi[b, at : at + PLANES * elem_rows, 128 * pair : 128 * pair + 128] = high
                    right_lo[b, at : at + PLANES * elem_rows, 128 * pair : 128 * pair + 128] = low
        traces.append(jnp.sum(energy))

    def project(step, carry):
        at = pl.ds(pl.multiple_of(step * ROWS, ROWS), ROWS)
        for b in range(2):
            proj = jnp.dot(left[b, at, : 2 * elems], right_hi[b], preferred_element_type=F32)
            proj += jnp.dot(left[b, at, : 2 * elems], right_lo[b], preferred_element_type=F32)
            proj += jnp.dot(left[b, at, 2 * elems :], right_hi[b], preferred_element_type=F32)
            square = proj * proj
            for piece in range(ROWS // 128):
                quads[b, pl.ds(step * (ROWS // 128) + piece, 1), :] = row_sums(square[128 * piece : 128 * piece + 128])
        return carry

    lax.fori_loop(0, grid_rows // ROWS, project, 0)

    snap_total = snap_rows * peers
    power = jnp.zeros((grid_rows // 128, 128), F32)
    for b in range(2):
        trace = traces[b] / snap_total + EPS
        power = power + quads[b] / snap_total / ((norms[b] + EPS) * trace / elems)
    power = power / bin_count
    for r in range(grid_rows // 128):
        shares[r] = power[r : r + 1]
    arrived[me] = shares[me // 2]

    def share_copy(other, source):
        return pltpu.make_async_remote_copy(
            src_ref=shares.at[other // 2], dst_ref=arrived.at[source], send_sem=share_send.at[other],
            recv_sem=share_recv.at[source], device_id={"tm": other, "rep": rep_at(column, plane)},
            device_id_type=MESH)

    def send_share(off, carry):
        share_copy(lax.rem(me + off, peers), me).start()
        return carry

    lax.fori_loop(1, peers, send_share, 0)

    def drain(off, carry):
        other = lax.rem(me + off, peers)
        piece_copy(other, me, column, column).wait_send()
        piece_copy(other, me, 1 - column, column).wait_send()
        share_copy(other, me).wait_send()
        return carry

    piece_copy(me, me, 1 - column, column).wait_send()
    lax.fori_loop(1, peers, drain, 0)
    for copy in started:
        copy.wait_send()

    def take_share(off, carry):
        other = lax.rem(me + off, peers)
        share_copy(other, other).wait_recv()
        return carry

    lax.fori_loop(1, peers, take_share, 0)
    total = jnp.sum(arrived[...], axis=0)
    odd = (me & 1) == 1
    out_ref[...] = jnp.where(odd, total[:, 64:], total[:, :64])


def shards(peers, snapshots, freq_bins, replicas):
    snap_rows, elem_rows, samples = snapshots.shape
    bins, grid_rows, elems = replicas.shape[1:]
    any_space = pl.BlockSpec(memory_space=pl.ANY)
    moves = 2 * PLANES
    out = pl.pallas_call(
        functools.partial(fused, peers),
        out_shape=jax.ShapeDtypeStruct((1, grid_rows // peers), F32),
        in_specs=[pl.BlockSpec(memory_space=pltpu.SMEM), any_space, any_space],
        out_specs=pl.BlockSpec(memory_space=pltpu.VMEM),
        scratch_shapes=[
            pltpu.VMEM(snapshots.shape, F32),
            pltpu.VMEM(replicas.shape, F32),
            pltpu.VMEM((samples, 128), BF16),
            pltpu.VMEM((peers, 8, 128), F32),
            pltpu.VMEM((COLUMNS, peers, 8, 128), F32),
            pltpu.VMEM((PLANES, COLUMNS, 4, 8, 128), F32),
            pltpu.VMEM((bins, grid_rows, 4 * elems), BF16),
            pltpu.VMEM((bins, 2 * elems, 256), BF16),
            pltpu.VMEM((bins, 2 * elems, 256), BF16),
            pltpu.VMEM((bins, grid_rows // 128, 128), F32),
            pltpu.VMEM((bins, grid_rows // 128, 128), F32),
            pltpu.VMEM((grid_rows // 128, 1, 128), F32),
            pltpu.VMEM((peers, 1, 128), F32),
            pltpu.SemaphoreType.DMA((3,)),
            pltpu.SemaphoreType.DMA((COLUMNS, peers)),
            pltpu.SemaphoreType.DMA((COLUMNS, peers)),
            pltpu.SemaphoreType.DMA((moves,)),
            pltpu.SemaphoreType.DMA((PLANES,)),
            pltpu.SemaphoreType.DMA((peers,)),
            pltpu.SemaphoreType.DMA((peers,)),
        ],
        compiler_params=pltpu.CompilerParams(collective_id=0, has_side_effects=True, vmem_limit_bytes=60 << 20),
    )(freq_bins, snapshots, replicas)
    return out.reshape(-1)


def solution(mesh):
    in_specs = (P("tm", "rep", None), P(), P(None, "tm", "rep", None))
    out_specs = P(("rep", "tm"))
    body = functools.partial(shards, mesh.shape["tm"])
    return jax.shard_map(body, mesh=mesh, in_specs=in_specs, out_specs=out_specs, check_vma=False)
```

```python
import functools
import math

import jax
import jax.numpy as jnp
from jax import lax
from jax.experimental import pallas as pl
from jax.experimental.pallas import tpu as pltpu
from jax.sharding import PartitionSpec as P

EPS = 1e-6
PLANES = 16
COLUMNS = 2
UP = {6: (2, 1, -1), 2: (2, 1, -1)}
DOWN = {5: (2, 1, -1), 2: (1, -1)}
ROWS = 256
MESH = pl.DeviceIdType.MESH
F32 = jnp.float32
BF16 = jnp.bfloat16


def split(value):
    high = value.astype(BF16)
    low = (value - high.astype(F32)).astype(BF16)
    return high, low


def lane_iota(shape):
    return lax.broadcasted_iota(jnp.int32, shape, len(shape) - 1)


def row_sums(value):
    return jnp.sum(value.T, axis=0, keepdims=True)


def fused(peers, bins_hbm, snaps_hbm, reps_hbm, out_ref, bins_ref, snaps, reps, table, pieces, landed, blocks, left_hi, left_lo, halves, right_hi,
          right_lo, norms, quads, shares, arrived, load_sem, piece_send, piece_recv, block_send, block_recv, share_send,
          share_recv, ready, cross_send, cross_recv):
    me = lax.axis_index("tm")
    spot = lax.axis_index("rep")
    column = spot // PLANES
    plane = spot % PLANES
    bin_count = bins_ref.shape[0]
    snap_rows, elem_rows, samples = snaps.shape
    grid_rows = reps.shape[2]
    elems = reps.shape[3]

    def rep_at(col, z):
        return col * PLANES + lax.rem(z + 2 * PLANES, PLANES)

    legs = set()
    for tree in (UP, DOWN):
        for hub, leaves in tree.items():
            legs |= {hub} | set(leaves)
    near = sorted(legs | {-d for d in legs})

    def plane_at(offset):
        return lax.rem(plane + offset + PLANES, PLANES)

    bins_load = pltpu.make_async_copy(bins_hbm, bins_ref, load_sem.at[3])
    bins_load.start()
    snap_load = pltpu.make_async_copy(snaps_hbm, snaps, load_sem.at[0])
    snap_load.start()
    rep_loads = [pltpu.make_async_copy(reps_hbm.at[:, b], reps.at[:, b], load_sem.at[1 + b]) for b in range(2)]
    for load in rep_loads:
        load.start()


    barrier = pltpu.get_barrier_semaphore()

    def greet(off, carry):
        other = lax.rem(me + off, peers)
        pl.semaphore_signal(barrier, inc=1, device_id={"tm": other, "rep": rep_at(column, plane)}, device_id_type=MESH)
        return carry

    lax.fori_loop(1, peers, greet, 0)
    pl.semaphore_signal(barrier, inc=1, device_id={"tm": me, "rep": rep_at(1 - column, plane)}, device_id_type=MESH)
    def rank(z):
        return jnp.where(z < PLANES // 2, z, 3 * PLANES // 2 - 1 - z)

    greeted = peers
    answers = 0
    for d in near:
        higher = rank(plane_at(d)) > rank(plane)

        @pl.when(higher)
        def _(d=d):
            pl.semaphore_signal(barrier, inc=1, device_id={"tm": me, "rep": rep_at(column, plane + d)},
                                device_id_type=MESH)

        greeted = greeted + jnp.where(higher, 0, 1)
        answers = answers + jnp.where(higher, 1, 0)

    lane = lane_iota((1, 128))
    bins_load.wait()
    chosen = jnp.zeros((1, 128), jnp.int32)
    for k in range(bin_count):
        chosen = jnp.where((lane & 63) // 2 == k, bins_ref[k], chosen)
    index = lax.broadcasted_iota(jnp.int32, (32, 128), 0)
    unit = 2.0 * math.pi / samples
    coarse = ((index * 32 * chosen) & (samples - 1)).astype(F32) * unit
    fine = ((index * chosen) & (samples - 1)).astype(F32) * unit
    cos_a, sin_a = jnp.cos(coarse), jnp.sin(coarse)
    cos_b, sin_b = jnp.cos(fine), jnp.sin(fine)
    real = (lane & 1) == 0
    with_cos = jnp.where(real, cos_b, -sin_b)
    with_sin = jnp.where(real, -sin_b, -cos_b)
    for a in range(samples // 32):
        rows = cos_a[a : a + 1] * with_cos + sin_a[a : a + 1] * with_sin
        high = rows.astype(BF16).astype(F32)
        table[32 * a : 32 * a + 32, :] = jnp.where(lane < 64, high, rows - high).astype(BF16)
    window = 0.5 - 0.5 * jnp.cos(lane_iota((1, samples)).astype(F32) * unit)

    quarter = me % 4
    wide = lane_iota((1, 4 * 128))
    owner = (wide // 128) * 4 + (((wide // 32) % 4 + 4 - quarter) & 3)
    key = owner * 4 + (wide // 8) % 4
    spread = (lax.broadcasted_iota(jnp.int32, (128, 512), 0) & 63 == key).astype(F32).astype(BF16)

    snap_load.wait()
    shaded = snaps[...].reshape(snap_rows * elem_rows, samples) * window
    high, low = split(shaded)
    spectra = jnp.dot(jnp.concatenate([high, low], axis=0), table[...], preferred_element_type=F32)
    high, low = split(spectra)
    placed = jnp.dot(jnp.concatenate([high, low], axis=0), spread, preferred_element_type=F32)
    slabs = jnp.sum(placed.reshape(4, snap_rows, elem_rows, 512), axis=0)
    merged = jnp.zeros((elem_rows, 512), F32)
    for s in range(snap_rows):
        merged = jnp.where((wide & 7) == s, slabs[s], merged)
    for tile in range(4):
        part = merged[:, 128 * tile : 128 * tile + 128]
        for d in range(4):
            pieces[4 * tile + d] = part if d == 0 else pltpu.roll(part, 128 - 32 * d, 1)
    landed[me] = pieces[me]

    pl.semaphore_wait(barrier, greeted)
    for d in near:
        @pl.when(rank(plane_at(d)) < rank(plane))
        def _(d=d):
            pl.semaphore_signal(ready, inc=1, device_id={"tm": me, "rep": rep_at(column, plane + d)},
                                device_id_type=MESH)

    def piece_copy(other, source):
        return pltpu.make_async_remote_copy(
            src_ref=pieces.at[other], dst_ref=landed.at[source], send_sem=piece_send,
            recv_sem=piece_recv, device_id={"tm": other, "rep": rep_at(column, plane)}, device_id_type=MESH)

    def send_piece(off, carry):
        piece_copy(lax.rem(me + off, peers), me).start()
        return carry

    lax.fori_loop(1, peers, send_piece, 0)

    near_lanes = pl.ds(pl.multiple_of(128 * column, 128), 128)
    far_lanes = pl.ds(pl.multiple_of(128 * (1 - column), 128), 128)
    for b in range(2):
        rep_loads[b].wait()

        def prepare(step, carry, b=b):
            at = pl.ds(pl.multiple_of(step * 128, 128), 128)
            energy = jnp.zeros((128, 128), F32)
            for part in range(2):
                for half, lanes in ((0, near_lanes), (1, far_lanes)):
                    value = reps[part, b, at, lanes]
                    high, low = split(value)
                    to = 256 * half + 128 * part
                    left_hi[b, at, to : to + 128] = high
                    left_lo[b, at, to : to + 128] = low
                    energy = energy + value * value
            norms[b, pl.ds(step, 1), :] = row_sums(energy)
            return carry

        lax.fori_loop(0, grid_rows // 128, prepare, 0)

    all_pieces = pltpu.make_async_remote_copy(
        src_ref=pieces.at[pl.ds(0, peers - 1)], dst_ref=landed.at[pl.ds(0, peers - 1)], send_sem=piece_send,
        recv_sem=piece_recv, device_id={"tm": lax.rem(me + 1, peers), "rep": spot}, device_id_type=MESH)
    all_pieces.wait_recv()

    tiles = []
    for tile in range(4):
        got = landed[4 * tile]
        for d in range(1, 4):
            got = jnp.where(lane // 32 == d, landed[4 * tile + d], got)
        tiles.append(got)
    for pair in range(2):
        first, second = tiles[2 * pair], tiles[2 * pair + 1]
        blocks[0, plane, pair] = jnp.where(lane & 16 == 0, first, pltpu.roll(second, 16, 1))
        blocks[0, plane, 2 + pair] = jnp.where(lane & 16 == 0, pltpu.roll(first, 112, 1), second)

    def block_copy(offset, to):
        owner_plane = plane_at(offset)
        return pltpu.make_async_remote_copy(
            src_ref=blocks.at[0, owner_plane], dst_ref=blocks.at[0, owner_plane], send_sem=block_send,
            recv_sem=block_recv.at[owner_plane], device_id={"tm": me, "rep": rep_at(column, plane + to)},
            device_id_type=MESH)

    def cross(offset):
        owner_plane = plane_at(offset)
        pltpu.make_async_remote_copy(
            src_ref=blocks.at[0, owner_plane], dst_ref=blocks.at[1, owner_plane], send_sem=cross_send,
            recv_sem=cross_recv, device_id={"tm": me, "rep": rep_at(1 - column, plane)}, device_id_type=MESH).start()

    sent = []

    def pass_on(offset, to):
        block_copy(offset, to).start()
        sent.append((offset, to))

    def take(offset):
        block_copy(offset, 1).wait_recv()

    turned_sign = (lane & 8) == 0
    energies = [jnp.zeros((8, 128), F32) for _ in range(2)]

    def build(half):
        count = PLANES * elem_rows
        for b in range(2):
            for pair in range(2):
                value = blocks[half, :, 2 * b + pair].reshape(count, 128)
                turned = jnp.where(turned_sign, pltpu.roll(value, 120, 1), -pltpu.roll(value, 8, 1))
                energies[b] = energies[b] + jnp.sum((value * value).reshape(count // 8, 8, 128), axis=0)
                for part, entry in ((0, value), (1, turned)):
                    high, low = split(entry)
                    at = 256 * half + 128 * part
                    right_hi[b, at : at + 128, 128 * pair : 128 * pair + 128] = high
                    right_lo[b, at : at + 128, 128 * pair : 128 * pair + 128] = low

    def product(b, at, half):
        k = slice(256 * half, 256 * half + 256)
        value = jnp.dot(left_hi[b, at, k], right_hi[b, k, :], preferred_element_type=F32)
        value += jnp.dot(left_hi[b, at, k], right_lo[b, k, :], preferred_element_type=F32)
        return value + jnp.dot(left_lo[b, at, k], right_hi[b, k, :], preferred_element_type=F32)

    cross(0)

    @pl.when(answers > 0)
    def _():
        pl.semaphore_wait(ready, answers)

    for hub in sorted(UP, reverse=True):
        pass_on(0, hub)
    for hub in sorted(DOWN, reverse=True):
        pass_on(0, -hub)
    hubs = sorted([(hub, -hub, 1, leaves) for hub, leaves in UP.items()]
                  + [(hub, hub, -1, leaves) for hub, leaves in DOWN.items()])
    rest = []
    for hub, offset, way, leaves in hubs:
        take(offset)
        for leaf in leaves:
            pass_on(offset, way * leaf)
        cross(offset)
        rest += [(hub + leaf, -way * (hub + leaf)) for leaf in leaves]
    for _, offset in sorted(rest):
        take(offset)
        cross(offset)
    assert len(rest) + len(hubs) == PLANES - 1
    build(0)

    def project_near(step, carry):
        at = pl.ds(pl.multiple_of(step * ROWS, ROWS), ROWS)
        for b in range(2):
            halves[b, at, :] = product(b, at, 0)
        return carry

    lax.fori_loop(0, grid_rows // ROWS, project_near, 0)
    all_crossed = pltpu.make_async_remote_copy(
        src_ref=blocks.at[0], dst_ref=blocks.at[1], send_sem=cross_send, recv_sem=cross_recv,
        device_id={"tm": me, "rep": rep_at(1 - column, plane)}, device_id_type=MESH)
    all_crossed.wait_recv()
    build(1)

    def project(step, carry):
        at = pl.ds(pl.multiple_of(step * ROWS, ROWS), ROWS)
        for b in range(2):
            proj = halves[b, at, :] + product(b, at, 1)
            square = proj * proj
            square = square[:, :128] + square[:, 128:]
            for piece in range(ROWS // 128):
                quads[b, pl.ds(step * (ROWS // 128) + piece, 1), :] = row_sums(square[128 * piece : 128 * piece + 128])
        return carry

    lax.fori_loop(0, grid_rows // ROWS, project, 0)
    traces = [jnp.sum(energy) for energy in energies]

    snap_total = snap_rows * peers
    power = jnp.zeros((grid_rows // 128, 128), F32)
    for b in range(2):
        trace = traces[b] / snap_total + EPS
        power = power + quads[b] / snap_total / ((norms[b] + EPS) * trace / elems)
    power = power / bin_count
    for r in range(grid_rows // 128):
        shares[r] = power[r : r + 1]
    arrived[me] = shares[me // 2]

    def send_share(off, carry):
        other = lax.rem(me + off, peers)
        pltpu.make_async_remote_copy(
            src_ref=shares.at[other // 2], dst_ref=arrived.at[me], send_sem=share_send, recv_sem=share_recv,
            device_id={"tm": other, "rep": spot}, device_id_type=MESH).start()
        return carry

    lax.fori_loop(1, peers, send_share, 0)
    all_pieces.wait_send()
    all_crossed.wait_send()
    pltpu.make_async_remote_copy(
        src_ref=blocks.at[0, pl.ds(0, PLANES - 1)], dst_ref=blocks.at[0, pl.ds(0, PLANES - 1)], send_sem=block_send,
        recv_sem=block_recv.at[plane], device_id={"tm": me, "rep": rep_at(column, plane + 1)},
        device_id_type=MESH).wait_send()
    assert len(sent) == PLANES - 1
    all_shares = pltpu.make_async_remote_copy(
        src_ref=arrived.at[pl.ds(0, peers - 1)], dst_ref=arrived.at[pl.ds(0, peers - 1)], send_sem=share_send,
        recv_sem=share_recv, device_id={"tm": lax.rem(me + 1, peers), "rep": spot}, device_id_type=MESH)
    all_shares.wait_send()
    all_shares.wait_recv()
    total = jnp.sum(arrived[...], axis=0)
    odd = (me & 1) == 1
    out_ref[...] = jnp.where(odd, total[:, 64:], total[:, :64])


def shards(peers, snapshots, freq_bins, replicas):
    snap_rows, elem_rows, samples = snapshots.shape
    bins, grid_rows, elems = replicas.shape[1:]
    any_space = pl.BlockSpec(memory_space=pltpu.HBM)
    out = pl.pallas_call(
        functools.partial(fused, peers),
        out_shape=pltpu.VMEM((1, grid_rows // peers), F32),
        in_specs=[any_space, any_space, any_space],
        out_specs=pl.BlockSpec(memory_space=pltpu.VMEM),
        scratch_shapes=[
            pltpu.SMEM(freq_bins.shape, jnp.int32),
            pltpu.VMEM(snapshots.shape, F32),
            pltpu.VMEM(replicas.shape, F32),
            pltpu.VMEM((samples, 128), BF16),
            pltpu.VMEM((peers, 8, 128), F32),
            pltpu.VMEM((peers, 8, 128), F32),
            pltpu.VMEM((COLUMNS, PLANES, 4, 8, 128), F32),
            pltpu.VMEM((bins, grid_rows, 2 * elems), BF16),
            pltpu.VMEM((bins, grid_rows, 2 * elems), BF16),
            pltpu.VMEM((bins, grid_rows, 256), F32),
            pltpu.VMEM((bins, 2 * elems, 256), BF16),
            pltpu.VMEM((bins, 2 * elems, 256), BF16),
            pltpu.VMEM((bins, grid_rows // 128, 128), F32),
            pltpu.VMEM((bins, grid_rows // 128, 128), F32),
            pltpu.VMEM((grid_rows // 128, 1, 128), F32),
            pltpu.VMEM((peers, 1, 128), F32),
            pltpu.SemaphoreType.DMA((4,)),
            pltpu.SemaphoreType.DMA,
            pltpu.SemaphoreType.DMA,
            pltpu.SemaphoreType.DMA,
            pltpu.SemaphoreType.DMA((PLANES,)),
            pltpu.SemaphoreType.DMA,
            pltpu.SemaphoreType.DMA,
            pltpu.SemaphoreType.REGULAR,
            pltpu.SemaphoreType.DMA,
            pltpu.SemaphoreType.DMA,
        ],
        compiler_params=pltpu.CompilerParams(collective_id=0, has_side_effects=True, vmem_limit_bytes=60 << 20),
    )(freq_bins, snapshots, replicas)
    return out.reshape(-1)


def solution(mesh):
    in_specs = (P("tm", "rep", None), P(), P(None, "tm", "rep", None))
    out_specs = P(("rep", "tm"))
    body = functools.partial(shards, mesh.shape["tm"])
    return jax.shard_map(body, mesh=mesh, in_specs=in_specs, out_specs=out_specs, check_vma=False)
```

```python
import functools
import math

import jax
import jax.numpy as jnp
from jax import lax
from jax.experimental import pallas as pl
from jax.experimental.pallas import tpu as pltpu
from jax.sharding import PartitionSpec as P

EPS = 1e-6
PLANES = 16
COLUMNS = 2
UP = {6: (2, 1, -1), 2: (2, 1, -1)}
DOWN = {5: (2, 1, -1), 2: (1, -1)}
LATE = 6
ROWS = 1024
MESH = pl.DeviceIdType.MESH
F32 = jnp.float32
BF16 = jnp.bfloat16


def split(value):
    high = value.astype(BF16)
    low = (value - high.astype(F32)).astype(BF16)
    return high, low


def lane_iota(shape):
    return lax.broadcasted_iota(jnp.int32, shape, len(shape) - 1)


def row_sums(value):
    return jnp.sum(value.T, axis=0, keepdims=True)


def fused(peers, bins_hbm, snaps_hbm, reps_hbm, out_ref, bins_ref, snaps, reps, table, pieces, landed, blocks, left_hi, left_lo, halves, right_hi,
          right_lo, norms, quads, shares, arrived, load_sem, piece_send, piece_recv, block_send, block_recv, share_send,
          share_recv, ready, cross_send, cross_recv, late_recv, late,
          left_late, right_late, window, spread):
    me = lax.axis_index("tm")
    spot = lax.axis_index("rep")
    column = spot // PLANES
    plane = spot % PLANES
    bin_count = bins_ref.shape[0]
    snap_rows, elem_rows, samples = snaps.shape
    grid_rows = reps.shape[2]
    elems = reps.shape[3]

    def rep_at(col, z):
        return col * PLANES + lax.rem(z + 2 * PLANES, PLANES)

    legs = set()
    for tree in (UP, DOWN):
        for hub, leaves in tree.items():
            legs |= {hub} | set(leaves)
    near = sorted(legs | {-d for d in legs})

    def plane_at(offset):
        return lax.rem(plane + offset + PLANES, PLANES)

    bins_load = pltpu.make_async_copy(bins_hbm, bins_ref, load_sem.at[3])
    bins_load.start()
    snap_load = pltpu.make_async_copy(snaps_hbm, snaps, load_sem.at[0])
    snap_load.start()
    rep_loads = [pltpu.make_async_copy(reps_hbm.at[:, b], reps.at[:, b], load_sem.at[1 + b]) for b in range(2)]
    for load in rep_loads:
        load.start()


    barrier = pltpu.get_barrier_semaphore()

    def greet(off, carry):
        other = lax.rem(me + off, peers)
        pl.semaphore_signal(barrier, inc=1, device_id={"tm": other, "rep": rep_at(column, plane)}, device_id_type=MESH)
        return carry

    lax.fori_loop(1, peers, greet, 0)
    pl.semaphore_signal(barrier, inc=1, device_id={"tm": me, "rep": rep_at(1 - column, plane)}, device_id_type=MESH)
    def rank(z):
        return jnp.where(z < PLANES // 2, z, 3 * PLANES // 2 - 1 - z)

    greeted = peers
    answers = 0
    for d in near:
        higher = rank(plane_at(d)) > rank(plane)

        @pl.when(higher)
        def _(d=d):
            pl.semaphore_signal(barrier, inc=1, device_id={"tm": me, "rep": rep_at(column, plane + d)},
                                device_id_type=MESH)

        greeted = greeted + jnp.where(higher, 0, 1)
        answers = answers + jnp.where(higher, 1, 0)

    lane = lane_iota((1, 128))
    unit = 2.0 * math.pi / samples
    window[...] = 0.5 - 0.5 * jnp.cos(lane_iota((1, samples)).astype(F32) * unit)
    wide = lane_iota((1, 4 * 128))
    quarter = me % 4
    owner = (wide // 128) * 4 + (((wide // 32) % 4 + 4 - quarter) & 3)
    key = owner * 4 + (wide // 8) % 4
    spread[...] = (lax.broadcasted_iota(jnp.int32, (128, 512), 0) & 63 == key).astype(F32).astype(BF16)

    for k in range(4):
        blocks[1, plane_at(LATE + k)] = jnp.zeros((4, 8, 128), F32)
    right_late[:, 192:, :] = jnp.zeros((2, 64, 256), BF16)
    bins_load.wait()
    chosen = jnp.zeros((1, 128), jnp.int32)
    for k in range(bin_count):
        chosen = jnp.where((lane & 63) // 2 == k, bins_ref[k], chosen)
    index = lax.broadcasted_iota(jnp.int32, (32, 128), 0)
    coarse = ((index * 32 * chosen) & (samples - 1)).astype(F32) * unit
    fine = ((index * chosen) & (samples - 1)).astype(F32) * unit
    cos_a, sin_a = jnp.cos(coarse), jnp.sin(coarse)
    cos_b, sin_b = jnp.cos(fine), jnp.sin(fine)
    real = (lane & 1) == 0
    with_cos = jnp.where(real, cos_b, -sin_b)
    with_sin = jnp.where(real, -sin_b, -cos_b)
    for a in range(samples // 32):
        rows = cos_a[a : a + 1] * with_cos + sin_a[a : a + 1] * with_sin
        high = rows.astype(BF16).astype(F32)
        table[32 * a : 32 * a + 32, :] = jnp.where(lane < 64, high, rows - high).astype(BF16)

    snap_load.wait()
    shaded = snaps[...].reshape(snap_rows * elem_rows, samples) * window[...]
    high, low = split(shaded)
    spectra = jnp.dot(jnp.concatenate([high, low], axis=0), table[...], preferred_element_type=F32)
    high, low = split(spectra)
    placed = jnp.dot(jnp.concatenate([high, low], axis=0), spread[...], preferred_element_type=F32)
    slabs = jnp.sum(placed.reshape(4, snap_rows, elem_rows, 512), axis=0)
    merged = jnp.zeros((elem_rows, 512), F32)
    for s in range(snap_rows):
        merged = jnp.where((wide & 7) == s, slabs[s], merged)
    for tile in range(4):
        part = merged[:, 128 * tile : 128 * tile + 128]
        for d in range(4):
            pieces[4 * tile + d] = part if d == 0 else pltpu.roll(part, 128 - 32 * d, 1)
    landed[me] = pieces[me]

    pl.semaphore_wait(barrier, greeted)
    for d in near:
        @pl.when(rank(plane_at(d)) < rank(plane))
        def _(d=d):
            pl.semaphore_signal(ready, inc=1, device_id={"tm": me, "rep": rep_at(column, plane + d)},
                                device_id_type=MESH)

    def piece_copy(other, source):
        return pltpu.make_async_remote_copy(
            src_ref=pieces.at[other], dst_ref=landed.at[source], send_sem=piece_send,
            recv_sem=piece_recv, device_id={"tm": other, "rep": rep_at(column, plane)}, device_id_type=MESH)

    def send_piece(off, carry):
        piece_copy(lax.rem(me + off, peers), me).start()
        return carry

    lax.fori_loop(1, peers, send_piece, 0)

    near_lanes = pl.ds(pl.multiple_of(128 * column, 128), 128)
    far_lanes = pl.ds(pl.multiple_of(128 * (1 - column), 128), 128)
    turn = (8 * (2 * PLANES - LATE - plane)) & 127
    turn_im = (turn + 32) & 127
    for b in range(2):
        rep_loads[b].wait()

        def prepare(step, carry, b=b):
            at = pl.ds(pl.multiple_of(step * 128, 128), 128)
            energy = jnp.zeros((128, 128), F32)
            parts = []
            for half, lanes in ((0, near_lanes), (1, far_lanes)):
                for part in range(2):
                    value = reps[part, b, at, lanes]
                    high, low = split(value)
                    to = 256 * half + 128 * part
                    left_hi[b, at, to : to + 128] = high
                    left_lo[b, at, to : to + 128] = low
                    energy = energy + value * value
                    parts.append(value)
            last = jnp.where(lane < 32, pltpu.roll(parts[2], turn, 1), pltpu.roll(parts[3], turn_im, 1))
            last = jnp.where(lane < 64, last, pltpu.roll(last, 64, 1))
            high, low = split(last)
            left_late[b, at, 0:128] = high
            left_late[b, at, 128:256] = low
            norms[b, pl.ds(step, 1), :] = row_sums(energy)
            return carry

        lax.fori_loop(0, grid_rows // 128, prepare, 0)

    all_pieces = pltpu.make_async_remote_copy(
        src_ref=pieces.at[pl.ds(0, peers - 1)], dst_ref=landed.at[pl.ds(0, peers - 1)], send_sem=piece_send,
        recv_sem=piece_recv, device_id={"tm": lax.rem(me + 1, peers), "rep": spot}, device_id_type=MESH)
    all_pieces.wait_recv()

    tiles = []
    for tile in range(4):
        got = landed[4 * tile]
        for d in range(1, 4):
            got = jnp.where(lane // 32 == d, landed[4 * tile + d], got)
        tiles.append(got)
    for pair in range(2):
        first, second = tiles[2 * pair], tiles[2 * pair + 1]
        blocks[0, plane, pair] = jnp.where(lane & 16 == 0, first, pltpu.roll(second, 16, 1))
        blocks[0, plane, 2 + pair] = jnp.where(lane & 16 == 0, pltpu.roll(first, 112, 1), second)

    def block_copy(offset, to):
        owner_plane = plane_at(offset)
        return pltpu.make_async_remote_copy(
            src_ref=blocks.at[0, owner_plane], dst_ref=blocks.at[0, owner_plane], send_sem=block_send,
            recv_sem=block_recv.at[owner_plane], device_id={"tm": me, "rep": rep_at(column, plane + to)},
            device_id_type=MESH)

    late_count = late.shape[0]

    def cross(offset):
        owner_plane = plane_at(offset)
        slot = (offset - LATE) % PLANES
        target, sem = (late.at[slot], late_recv) if slot < late_count else (blocks.at[1, owner_plane], cross_recv)
        pltpu.make_async_remote_copy(
            src_ref=blocks.at[0, owner_plane], dst_ref=target, send_sem=cross_send, recv_sem=sem,
            device_id={"tm": me, "rep": rep_at(1 - column, plane)}, device_id_type=MESH).start()

    sent = []

    def pass_on(offset, to):
        block_copy(offset, to).start()
        sent.append((offset, to))

    def take(offset):
        block_copy(offset, 1).wait_recv()

    turned_sign = (lane & 8) == 0
    energies = [jnp.zeros((8, 128), F32) for _ in range(2)]

    def halves_of(value, b):
        turned = jnp.where(turned_sign, pltpu.roll(value, 120, 1), -pltpu.roll(value, 8, 1))
        energies[b] = energies[b] + jnp.sum((value * value).reshape(-1, 8, 128), axis=0)
        return split(value) + split(turned)

    def build(half):
        for b in range(2):
            for pair in range(2):
                to = slice(128 * pair, 128 * pair + 128)
                high, low, turned_high, turned_low = halves_of(
                    blocks[half, :, 2 * b + pair].reshape(PLANES * elem_rows, 128), b)
                at = 256 * half
                right_hi[b, at : at + 128, to] = high
                right_lo[b, at : at + 128, to] = low
                right_hi[b, at + 128 : at + 256, to] = turned_high
                right_lo[b, at + 128 : at + 256, to] = turned_low

    def build_late():
        for b in range(2):
            for pair in range(2):
                to = slice(128 * pair, 128 * pair + 128)
                high, low, turned_high, turned_low = halves_of(
                    late[:, 2 * b + pair].reshape(late_count * elem_rows, 128), b)
                for at, entry in enumerate((high, turned_high, low, turned_low, high, turned_high)):
                    right_late[b, 32 * at : 32 * at + 32, to] = entry

    def product(b, at, half):
        k = slice(256 * half, 256 * half + 256)
        value = jnp.dot(left_hi[b, at, k], right_hi[b, k, :], preferred_element_type=F32)
        value += jnp.dot(left_hi[b, at, k], right_lo[b, k, :], preferred_element_type=F32)
        return value + jnp.dot(left_lo[b, at, k], right_hi[b, k, :], preferred_element_type=F32)

    cross(0)

    @pl.when(answers > 0)
    def _():
        pl.semaphore_wait(ready, answers)

    for hub in sorted(UP, reverse=True):
        pass_on(0, hub)
    for hub in sorted(DOWN, reverse=True):
        pass_on(0, -hub)
    hubs = sorted([(hub, -hub, 1, leaves) for hub, leaves in UP.items()]
                  + [(hub, hub, -1, leaves) for hub, leaves in DOWN.items()])
    rest = []
    for hub, offset, way, leaves in hubs:
        take(offset)
        for leaf in leaves:
            pass_on(offset, way * leaf)
        cross(offset)
        rest += [(hub + leaf, -way * (hub + leaf)) for leaf in leaves]
    for _, offset in sorted(rest):
        take(offset)
        cross(offset)
    assert len(rest) + len(hubs) == PLANES - 1
    build(0)

    def project_near(step, carry):
        at = pl.ds(pl.multiple_of(step * ROWS, ROWS), ROWS)
        for b in range(2):
            halves[b, at, :] = product(b, at, 0)
        return carry

    lax.fori_loop(0, grid_rows // ROWS, project_near, 0)
    all_crossed = pltpu.make_async_remote_copy(
        src_ref=blocks.at[0], dst_ref=blocks.at[1], send_sem=cross_send, recv_sem=cross_recv,
        device_id={"tm": me, "rep": rep_at(1 - column, plane)}, device_id_type=MESH)
    early_crossed = pltpu.make_async_remote_copy(
        src_ref=blocks.at[0, pl.ds(0, PLANES - late_count)], dst_ref=blocks.at[1, pl.ds(0, PLANES - late_count)],
        send_sem=cross_send, recv_sem=cross_recv, device_id={"tm": me, "rep": rep_at(1 - column, plane)},
        device_id_type=MESH)
    late_crossed = pltpu.make_async_remote_copy(
        src_ref=late, dst_ref=late, send_sem=cross_send, recv_sem=late_recv,
        device_id={"tm": me, "rep": rep_at(1 - column, plane)}, device_id_type=MESH)
    early_crossed.wait_recv()
    build(1)

    def project_far(step, carry):
        at = pl.ds(pl.multiple_of(step * ROWS, ROWS), ROWS)
        for b in range(2):
            halves[b, at, :] += product(b, at, 1)
        return carry

    lax.fori_loop(0, grid_rows // ROWS, project_far, 0)
    late_crossed.wait_recv()
    build_late()

    def project(step, carry):
        at = pl.ds(pl.multiple_of(step * ROWS, ROWS), ROWS)
        for b in range(2):
            proj = halves[b, at, :] + jnp.dot(left_late[b, at, :], right_late[b], preferred_element_type=F32)
            square = proj * proj
            square = square[:, :128] + square[:, 128:]
            for piece in range(ROWS // 128):
                quads[b, pl.ds(step * (ROWS // 128) + piece, 1), :] = row_sums(square[128 * piece : 128 * piece + 128])
        return carry

    lax.fori_loop(0, grid_rows // ROWS, project, 0)
    traces = [jnp.sum(energy) for energy in energies]

    snap_total = snap_rows * peers
    power = jnp.zeros((grid_rows // 128, 128), F32)
    for b in range(2):
        trace = traces[b] / snap_total + EPS
        power = power + quads[b] / snap_total / ((norms[b] + EPS) * trace / elems)
    power = power / bin_count
    for r in range(grid_rows // 128):
        shares[r] = power[r : r + 1]
    arrived[me] = shares[me // 2]

    def send_share(off, carry):
        other = lax.rem(me + off, peers)
        pltpu.make_async_remote_copy(
            src_ref=shares.at[other // 2], dst_ref=arrived.at[me], send_sem=share_send, recv_sem=share_recv,
            device_id={"tm": other, "rep": spot}, device_id_type=MESH).start()
        return carry

    lax.fori_loop(1, peers, send_share, 0)
    all_pieces.wait_send()
    all_crossed.wait_send()
    pltpu.make_async_remote_copy(
        src_ref=blocks.at[0, pl.ds(0, PLANES - 1)], dst_ref=blocks.at[0, pl.ds(0, PLANES - 1)], send_sem=block_send,
        recv_sem=block_recv.at[plane], device_id={"tm": me, "rep": rep_at(column, plane + 1)},
        device_id_type=MESH).wait_send()
    assert len(sent) == PLANES - 1
    all_shares = pltpu.make_async_remote_copy(
        src_ref=arrived.at[pl.ds(0, peers - 1)], dst_ref=arrived.at[pl.ds(0, peers - 1)], send_sem=share_send,
        recv_sem=share_recv, device_id={"tm": lax.rem(me + 1, peers), "rep": spot}, device_id_type=MESH)
    all_shares.wait_send()
    all_shares.wait_recv()
    total = jnp.sum(arrived[...], axis=0)
    odd = (me & 1) == 1
    out_ref[...] = jnp.where(odd, total[:, 64:], total[:, :64])


def shards(peers, snapshots, freq_bins, replicas):
    snap_rows, elem_rows, samples = snapshots.shape
    bins, grid_rows, elems = replicas.shape[1:]
    any_space = pl.BlockSpec(memory_space=pltpu.HBM)
    out = pl.pallas_call(
        functools.partial(fused, peers),
        out_shape=pltpu.VMEM((1, grid_rows // peers), F32),
        in_specs=[any_space, any_space, any_space],
        out_specs=pl.BlockSpec(memory_space=pltpu.VMEM),
        scratch_shapes=[
            pltpu.SMEM(freq_bins.shape, jnp.int32),
            pltpu.VMEM(snapshots.shape, F32),
            pltpu.VMEM(replicas.shape, F32),
            pltpu.VMEM((samples, 128), BF16),
            pltpu.VMEM((peers, 8, 128), F32),
            pltpu.VMEM((peers, 8, 128), F32),
            pltpu.VMEM((COLUMNS, PLANES, 4, 8, 128), F32),
            pltpu.VMEM((bins, grid_rows, 2 * elems), BF16),
            pltpu.VMEM((bins, grid_rows, 2 * elems), BF16),
            pltpu.VMEM((bins, grid_rows, 256), F32),
            pltpu.VMEM((bins, 2 * elems, 256), BF16),
            pltpu.VMEM((bins, 2 * elems, 256), BF16),
            pltpu.VMEM((bins, grid_rows // 128, 128), F32),
            pltpu.VMEM((bins, grid_rows // 128, 128), F32),
            pltpu.VMEM((grid_rows // 128, 1, 128), F32),
            pltpu.VMEM((peers, 1, 128), F32),
            pltpu.SemaphoreType.DMA((4,)),
            pltpu.SemaphoreType.DMA,
            pltpu.SemaphoreType.DMA,
            pltpu.SemaphoreType.DMA,
            pltpu.SemaphoreType.DMA((PLANES,)),
            pltpu.SemaphoreType.DMA,
            pltpu.SemaphoreType.DMA,
            pltpu.SemaphoreType.REGULAR,
            pltpu.SemaphoreType.DMA,
            pltpu.SemaphoreType.DMA,
            pltpu.SemaphoreType.DMA,
            pltpu.VMEM((4, 4, 8, 128), F32),
            pltpu.VMEM((bins, grid_rows, 256), BF16),
            pltpu.VMEM((bins, 256, 256), BF16),
            pltpu.VMEM((1, samples), F32),
            pltpu.VMEM((128, 512), BF16),
        ],
        compiler_params=pltpu.CompilerParams(collective_id=0, has_side_effects=True, vmem_limit_bytes=60 << 20),
    )(freq_bins, snapshots, replicas)
    return out.reshape(-1)


def solution(mesh):
    in_specs = (P("tm", "rep", None), P(), P(None, "tm", "rep", None))
    out_specs = P(("rep", "tm"))
    body = functools.partial(shards, mesh.shape["tm"])
    return jax.shard_map(body, mesh=mesh, in_specs=in_specs, out_specs=out_specs, check_vma=False)
```

```python
import functools
import math

import jax
import jax.numpy as jnp
from jax import lax
from jax.experimental import pallas as pl
from jax.experimental.pallas import tpu as pltpu
from jax.sharding import PartitionSpec as P

EPS = 1e-6
PLANES = 16
COLUMNS = 2
UP = {6: (2, 1, -1), 2: (2, 1, -1)}
DOWN = {5: (2, 1, -1), 2: (1, -1)}
LATE = 6
ROWS = 1024
MESH = pl.DeviceIdType.MESH
F32 = jnp.float32
BF16 = jnp.bfloat16


def split(value):
    high = value.astype(BF16)
    low = (value - high.astype(F32)).astype(BF16)
    return high, low


def lane_iota(shape):
    return lax.broadcasted_iota(jnp.int32, shape, len(shape) - 1)


def row_sums(value):
    return jnp.sum(value.T, axis=0, keepdims=True)


def fused(peers, bins_hbm, snaps_hbm, reps_hbm, out_ref, bins_ref, snaps, reps, table, pieces, landed, blocks, left_hi, left_lo, halves, right_hi,
          right_lo, norms, quads, shares, arrived, load_sem, piece_send, piece_recv, block_send, block_recv, share_send,
          share_recv, ready, cross_send, cross_recv, late_recv, late,
          left_late, right_late, window, spread):
    me = lax.axis_index("tm")
    spot = lax.axis_index("rep")
    column = spot // PLANES
    plane = spot % PLANES
    bin_count = bins_ref.shape[0]
    snap_rows, elem_rows, samples = snaps.shape
    grid_rows = reps.shape[2]
    elems = reps.shape[3]

    def rep_at(col, z):
        return col * PLANES + lax.rem(z + 2 * PLANES, PLANES)

    legs = set()
    for tree in (UP, DOWN):
        for hub, leaves in tree.items():
            legs |= {hub} | set(leaves)
    near = [(d, 0) for d in sorted(legs | {-d for d in legs})]
    diagonal = {leaf for tree in (UP, DOWN) for hub, leaves in tree.items() if hub > 0 for leaf in leaves}
    near += [(d, 1) for d in sorted(diagonal | {-d for d in diagonal})]

    def side(other):
        return 1 - column if other else column


    def plane_at(offset):
        return lax.rem(plane + offset + PLANES, PLANES)

    bins_load = pltpu.make_async_copy(bins_hbm, bins_ref, load_sem.at[3])
    bins_load.start()
    snap_load = pltpu.make_async_copy(snaps_hbm, snaps, load_sem.at[0])
    snap_load.start()
    rep_loads = [pltpu.make_async_copy(reps_hbm.at[:, b], reps.at[:, b], load_sem.at[1 + b]) for b in range(2)]
    for load in rep_loads:
        load.start()


    barrier = pltpu.get_barrier_semaphore()

    def greet(off, carry):
        other = lax.rem(me + off, peers)
        pl.semaphore_signal(barrier, inc=1, device_id={"tm": other, "rep": rep_at(column, plane)}, device_id_type=MESH)
        return carry

    lax.fori_loop(1, peers, greet, 0)
    pl.semaphore_signal(barrier, inc=1, device_id={"tm": me, "rep": rep_at(1 - column, plane)}, device_id_type=MESH)
    def rank(z):
        return jnp.where(z < PLANES // 2, z, 3 * PLANES // 2 - 1 - z)

    greeted = peers
    answers = 0
    for d, other in near:
        higher = rank(plane_at(d)) > rank(plane)

        @pl.when(higher)
        def _(d=d, other=other):
            pl.semaphore_signal(barrier, inc=1, device_id={"tm": me, "rep": rep_at(side(other), plane + d)},
                                device_id_type=MESH)

        greeted = greeted + jnp.where(higher, 0, 1)
        answers = answers + jnp.where(higher, 1, 0)

    lane = lane_iota((1, 128))
    unit = 2.0 * math.pi / samples
    window[...] = 0.5 - 0.5 * jnp.cos(lane_iota((1, samples)).astype(F32) * unit)
    wide = lane_iota((1, 4 * 128))
    quarter = me % 4
    owner = (wide // 128) * 4 + (((wide // 32) % 4 + 4 - quarter) & 3)
    key = owner * 4 + (wide // 8) % 4
    spread[...] = (lax.broadcasted_iota(jnp.int32, (128, 512), 0) & 63 == key).astype(F32).astype(BF16)

    for k in range(4):
        blocks[1, plane_at(LATE + k)] = jnp.zeros((4, 8, 128), F32)
    right_late[:, 192:, :] = jnp.zeros((2, 64, 256), BF16)
    bins_load.wait()
    chosen = jnp.zeros((1, 128), jnp.int32)
    for k in range(bin_count):
        chosen = jnp.where((lane & 63) // 2 == k, bins_ref[k], chosen)
    index = lax.broadcasted_iota(jnp.int32, (32, 128), 0)
    coarse = ((index * 32 * chosen) & (samples - 1)).astype(F32) * unit
    fine = ((index * chosen) & (samples - 1)).astype(F32) * unit
    cos_a, sin_a = jnp.cos(coarse), jnp.sin(coarse)
    cos_b, sin_b = jnp.cos(fine), jnp.sin(fine)
    real = (lane & 1) == 0
    with_cos = jnp.where(real, cos_b, -sin_b)
    with_sin = jnp.where(real, -sin_b, -cos_b)
    for a in range(samples // 32):
        rows = cos_a[a : a + 1] * with_cos + sin_a[a : a + 1] * with_sin
        high = rows.astype(BF16).astype(F32)
        table[32 * a : 32 * a + 32, :] = jnp.where(lane < 64, high, rows - high).astype(BF16)

    snap_load.wait()
    shaded = snaps[...].reshape(snap_rows * elem_rows, samples) * window[...]
    high, low = split(shaded)
    spectra = jnp.dot(jnp.concatenate([high, low], axis=0), table[...], preferred_element_type=F32)
    high, low = split(spectra)
    placed = jnp.dot(jnp.concatenate([high, low], axis=0), spread[...], preferred_element_type=F32)
    slabs = jnp.sum(placed.reshape(4, snap_rows, elem_rows, 512), axis=0)
    merged = jnp.zeros((elem_rows, 512), F32)
    for s in range(snap_rows):
        merged = jnp.where((wide & 7) == s, slabs[s], merged)
    for tile in range(4):
        part = merged[:, 128 * tile : 128 * tile + 128]
        for d in range(4):
            pieces[4 * tile + d] = part if d == 0 else pltpu.roll(part, 128 - 32 * d, 1)
    landed[me] = pieces[me]

    pl.semaphore_wait(barrier, greeted)
    for d, other in near:
        @pl.when(rank(plane_at(d)) < rank(plane))
        def _(d=d, other=other):
            pl.semaphore_signal(ready, inc=1, device_id={"tm": me, "rep": rep_at(side(other), plane + d)},
                                device_id_type=MESH)

    def piece_copy(other, source):
        return pltpu.make_async_remote_copy(
            src_ref=pieces.at[other], dst_ref=landed.at[source], send_sem=piece_send,
            recv_sem=piece_recv, device_id={"tm": other, "rep": rep_at(column, plane)}, device_id_type=MESH)

    def send_piece(off, carry):
        piece_copy(lax.rem(me + 1 + lax.rem(off + 10, peers - 1), peers), me).start()
        return carry

    lax.fori_loop(1, peers, send_piece, 0)

    near_lanes = pl.ds(pl.multiple_of(128 * column, 128), 128)
    far_lanes = pl.ds(pl.multiple_of(128 * (1 - column), 128), 128)
    turn = (8 * (2 * PLANES - LATE - plane)) & 127
    turn_im = (turn + 32) & 127
    for b in range(2):
        rep_loads[b].wait()

        def prepare(step, carry, b=b):
            at = pl.ds(pl.multiple_of(step * 128, 128), 128)
            energy = jnp.zeros((128, 128), F32)
            parts = []
            for half, lanes in ((0, near_lanes), (1, far_lanes)):
                for part in range(2):
                    value = reps[part, b, at, lanes]
                    high, low = split(value)
                    to = 256 * half + 128 * part
                    left_hi[b, at, to : to + 128] = high
                    left_lo[b, at, to : to + 128] = low
                    energy = energy + value * value
                    parts.append(value)
            last = jnp.where(lane < 32, pltpu.roll(parts[2], turn, 1), pltpu.roll(parts[3], turn_im, 1))
            last = jnp.where(lane < 64, last, pltpu.roll(last, 64, 1))
            high, low = split(last)
            left_late[b, at, 0:128] = high
            left_late[b, at, 128:256] = low
            norms[b, pl.ds(step, 1), :] = row_sums(energy)
            return carry

        lax.fori_loop(0, grid_rows // 128, prepare, 0)

    all_pieces = pltpu.make_async_remote_copy(
        src_ref=pieces.at[pl.ds(0, peers - 1)], dst_ref=landed.at[pl.ds(0, peers - 1)], send_sem=piece_send,
        recv_sem=piece_recv, device_id={"tm": lax.rem(me + 1, peers), "rep": spot}, device_id_type=MESH)
    all_pieces.wait_recv()

    tiles = []
    for tile in range(4):
        got = landed[4 * tile]
        for d in range(1, 4):
            got = jnp.where(lane // 32 == d, landed[4 * tile + d], got)
        tiles.append(got)
    for pair in range(2):
        first, second = tiles[2 * pair], tiles[2 * pair + 1]
        blocks[0, plane, pair] = jnp.where(lane & 16 == 0, first, pltpu.roll(second, 16, 1))
        blocks[0, plane, 2 + pair] = jnp.where(lane & 16 == 0, pltpu.roll(first, 112, 1), second)

    def block_copy(offset, to):
        owner_plane = plane_at(offset)
        return pltpu.make_async_remote_copy(
            src_ref=blocks.at[0, owner_plane], dst_ref=blocks.at[0, owner_plane], send_sem=block_send,
            recv_sem=block_recv.at[owner_plane], device_id={"tm": me, "rep": rep_at(column, plane + to)},
            device_id_type=MESH)

    late_count = late.shape[0]

    def cross(offset, to=0):
        owner_plane = plane_at(offset)
        slot = (offset - to - LATE) % PLANES
        target, sem = (late.at[slot], late_recv) if slot < late_count else (blocks.at[1, owner_plane], cross_recv)
        pltpu.make_async_remote_copy(
            src_ref=blocks.at[0, owner_plane], dst_ref=target, send_sem=cross_send, recv_sem=sem,
            device_id={"tm": me, "rep": rep_at(1 - column, plane + to)}, device_id_type=MESH).start()
        crossed.append((offset, to))

    crossed = []
    sent = []

    def pass_on(offset, to):
        block_copy(offset, to).start()
        sent.append((offset, to))

    def take(offset):
        block_copy(offset, 1).wait_recv()

    turned_sign = (lane & 8) == 0
    energies = [jnp.zeros((8, 128), F32) for _ in range(2)]

    def halves_of(value, b):
        turned = jnp.where(turned_sign, pltpu.roll(value, 120, 1), -pltpu.roll(value, 8, 1))
        energies[b] = energies[b] + jnp.sum((value * value).reshape(-1, 8, 128), axis=0)
        return split(value) + split(turned)

    def build(half):
        for b in range(2):
            for pair in range(2):
                to = slice(128 * pair, 128 * pair + 128)
                high, low, turned_high, turned_low = halves_of(
                    blocks[half, :, 2 * b + pair].reshape(PLANES * elem_rows, 128), b)
                at = 256 * half
                right_hi[b, at : at + 128, to] = high
                right_lo[b, at : at + 128, to] = low
                right_hi[b, at + 128 : at + 256, to] = turned_high
                right_lo[b, at + 128 : at + 256, to] = turned_low

    def build_late():
        for b in range(2):
            for pair in range(2):
                to = slice(128 * pair, 128 * pair + 128)
                high, low, turned_high, turned_low = halves_of(
                    late[:, 2 * b + pair].reshape(late_count * elem_rows, 128), b)
                for at, entry in enumerate((high, turned_high, low, turned_low, high, turned_high)):
                    right_late[b, 32 * at : 32 * at + 32, to] = entry

    def product(b, at, half):
        k = slice(256 * half, 256 * half + 256)
        value = jnp.dot(left_hi[b, at, k], right_hi[b, k, :], preferred_element_type=F32)
        value += jnp.dot(left_hi[b, at, k], right_lo[b, k, :], preferred_element_type=F32)
        return value + jnp.dot(left_lo[b, at, k], right_hi[b, k, :], preferred_element_type=F32)

    cross(0)

    @pl.when(answers > 0)
    def _():
        pl.semaphore_wait(ready, answers)

    for hub in sorted(UP, reverse=True):
        pass_on(0, hub)
    for hub in sorted(DOWN, reverse=True):
        pass_on(0, -hub)
    hubs = sorted([(hub, -hub, 1, leaves) for hub, leaves in UP.items()]
                  + [(hub, hub, -1, leaves) for hub, leaves in DOWN.items()])
    rest = []
    for hub, offset, way, leaves in hubs:
        take(offset)
        for leaf in leaves:
            pass_on(offset, way * leaf)
        if hub > 0:
            for leaf in leaves:
                cross(offset, way * leaf)
        cross(offset)
        rest += [(hub + leaf, -way * (hub + leaf), hub > 0) for leaf in leaves]
    for _, offset, done in sorted(rest):
        take(offset)
        if not done:
            cross(offset)
    assert len(crossed) == PLANES
    assert len(rest) + len(hubs) == PLANES - 1
    build(0)

    def project_near(step, carry):
        at = pl.ds(pl.multiple_of(step * ROWS, ROWS), ROWS)
        for b in range(2):
            halves[b, at, :] = product(b, at, 0)
        return carry

    lax.fori_loop(0, grid_rows // ROWS, project_near, 0)
    all_crossed = pltpu.make_async_remote_copy(
        src_ref=blocks.at[0], dst_ref=blocks.at[1], send_sem=cross_send, recv_sem=cross_recv,
        device_id={"tm": me, "rep": rep_at(1 - column, plane)}, device_id_type=MESH)
    early_crossed = pltpu.make_async_remote_copy(
        src_ref=blocks.at[0, pl.ds(0, PLANES - late_count)], dst_ref=blocks.at[1, pl.ds(0, PLANES - late_count)],
        send_sem=cross_send, recv_sem=cross_recv, device_id={"tm": me, "rep": rep_at(1 - column, plane)},
        device_id_type=MESH)
    late_crossed = pltpu.make_async_remote_copy(
        src_ref=late, dst_ref=late, send_sem=cross_send, recv_sem=late_recv,
        device_id={"tm": me, "rep": rep_at(1 - column, plane)}, device_id_type=MESH)
    early_crossed.wait_recv()
    build(1)

    def project_far(step, carry):
        at = pl.ds(pl.multiple_of(step * ROWS, ROWS), ROWS)
        for b in range(2):
            halves[b, at, :] += product(b, at, 1)
        return carry

    lax.fori_loop(0, grid_rows // ROWS, project_far, 0)
    late_crossed.wait_recv()
    build_late()

    def project(step, carry):
        at = pl.ds(pl.multiple_of(step * ROWS, ROWS), ROWS)
        for b in range(2):
            proj = halves[b, at, :] + jnp.dot(left_late[b, at, :], right_late[b], preferred_element_type=F32)
            square = proj * proj
            square = square[:, :128] + square[:, 128:]
            for piece in range(ROWS // 128):
                quads[b, pl.ds(step * (ROWS // 128) + piece, 1), :] = row_sums(square[128 * piece : 128 * piece + 128])
        return carry

    lax.fori_loop(0, grid_rows // ROWS, project, 0)
    traces = [jnp.sum(energy) for energy in energies]

    snap_total = snap_rows * peers
    power = jnp.zeros((grid_rows // 128, 128), F32)
    for b in range(2):
        trace = traces[b] / snap_total + EPS
        power = power + quads[b] / snap_total / ((norms[b] + EPS) * trace / elems)
    power = power / bin_count
    for r in range(grid_rows // 128):
        shares[r] = power[r : r + 1]
    arrived[me] = shares[me // 2]

    def send_share(off, carry):
        other = lax.rem(me + 1 + lax.rem(off + 10, peers - 1), peers)
        pltpu.make_async_remote_copy(
            src_ref=shares.at[other // 2], dst_ref=arrived.at[me], send_sem=share_send, recv_sem=share_recv,
            device_id={"tm": other, "rep": spot}, device_id_type=MESH).start()
        return carry

    lax.fori_loop(1, peers, send_share, 0)
    all_pieces.wait_send()
    all_crossed.wait_send()
    pltpu.make_async_remote_copy(
        src_ref=blocks.at[0, pl.ds(0, PLANES - 1)], dst_ref=blocks.at[0, pl.ds(0, PLANES - 1)], send_sem=block_send,
        recv_sem=block_recv.at[plane], device_id={"tm": me, "rep": rep_at(column, plane + 1)},
        device_id_type=MESH).wait_send()
    assert len(sent) == PLANES - 1
    all_shares = pltpu.make_async_remote_copy(
        src_ref=arrived.at[pl.ds(0, peers - 1)], dst_ref=arrived.at[pl.ds(0, peers - 1)], send_sem=share_send,
        recv_sem=share_recv, device_id={"tm": lax.rem(me + 1, peers), "rep": spot}, device_id_type=MESH)
    all_shares.wait_send()
    all_shares.wait_recv()
    total = jnp.sum(arrived[...], axis=0)
    odd = (me & 1) == 1
    out_ref[...] = jnp.where(odd, total[:, 64:], total[:, :64])


def shards(peers, snapshots, freq_bins, replicas):
    snap_rows, elem_rows, samples = snapshots.shape
    bins, grid_rows, elems = replicas.shape[1:]
    any_space = pl.BlockSpec(memory_space=pltpu.HBM)
    out = pl.pallas_call(
        functools.partial(fused, peers),
        out_shape=pltpu.VMEM((1, grid_rows // peers), F32),
        in_specs=[any_space, any_space, any_space],
        out_specs=pl.BlockSpec(memory_space=pltpu.VMEM),
        scratch_shapes=[
            pltpu.SMEM(freq_bins.shape, jnp.int32),
            pltpu.VMEM(snapshots.shape, F32),
            pltpu.VMEM(replicas.shape, F32),
            pltpu.VMEM((samples, 128), BF16),
            pltpu.VMEM((peers, 8, 128), F32),
            pltpu.VMEM((peers, 8, 128), F32),
            pltpu.VMEM((COLUMNS, PLANES, 4, 8, 128), F32),
            pltpu.VMEM((bins, grid_rows, 2 * elems), BF16),
            pltpu.VMEM((bins, grid_rows, 2 * elems), BF16),
            pltpu.VMEM((bins, grid_rows, 256), F32),
            pltpu.VMEM((bins, 2 * elems, 256), BF16),
            pltpu.VMEM((bins, 2 * elems, 256), BF16),
            pltpu.VMEM((bins, grid_rows // 128, 128), F32),
            pltpu.VMEM((bins, grid_rows // 128, 128), F32),
            pltpu.VMEM((grid_rows // 128, 1, 128), F32),
            pltpu.VMEM((peers, 1, 128), F32),
            pltpu.SemaphoreType.DMA((4,)),
            pltpu.SemaphoreType.DMA,
            pltpu.SemaphoreType.DMA,
            pltpu.SemaphoreType.DMA,
            pltpu.SemaphoreType.DMA((PLANES,)),
            pltpu.SemaphoreType.DMA,
            pltpu.SemaphoreType.DMA,
            pltpu.SemaphoreType.REGULAR,
            pltpu.SemaphoreType.DMA,
            pltpu.SemaphoreType.DMA,
            pltpu.SemaphoreType.DMA,
            pltpu.VMEM((4, 4, 8, 128), F32),
            pltpu.VMEM((bins, grid_rows, 256), BF16),
            pltpu.VMEM((bins, 256, 256), BF16),
            pltpu.VMEM((1, samples), F32),
            pltpu.VMEM((128, 512), BF16),
        ],
        compiler_params=pltpu.CompilerParams(collective_id=0, has_side_effects=True, vmem_limit_bytes=60 << 20),
    )(freq_bins, snapshots, replicas)
    return out.reshape(-1)


def solution(mesh):
    in_specs = (P("tm", "rep", None), P(), P(None, "tm", "rep", None))
    out_specs = P(("rep", "tm"))
    body = functools.partial(shards, mesh.shape["tm"])
    return jax.shard_map(body, mesh=mesh, in_specs=in_specs, out_specs=out_specs, check_vma=False)
```

```python
import functools
import math

import jax
import jax.numpy as jnp
from jax import lax
from jax.experimental import pallas as pl
from jax.experimental.pallas import tpu as pltpu
from jax.sharding import PartitionSpec as P

EPS = 1e-6
PLANES = 16
COLUMNS = 2
UP = {6: (2, 1, -1), 2: (2, 1, -1)}
DOWN = {5: (2, 1, -1), 2: (1, -1)}
LATE = 6
ROWS = 1024
MESH = pl.DeviceIdType.MESH
F32 = jnp.float32
BF16 = jnp.bfloat16


def split(value):
    high = value.astype(BF16)
    low = (value - high.astype(F32)).astype(BF16)
    return high, low


def lane_iota(shape):
    return lax.broadcasted_iota(jnp.int32, shape, len(shape) - 1)


def row_sums(value):
    return jnp.sum(value.T, axis=0, keepdims=True)


def fused(peers, bins_hbm, snaps_hbm, reps_hbm, out_ref, bins_ref, snaps, reps, table, pieces, landed, blocks, left_hi, left_lo, halves, right_hi,
          right_lo, norms, quads, shares, arrived, load_sem, piece_send, piece_recv, block_send, block_recv, share_send,
          share_recv, ready, cross_send, cross_recv, late_recv, late,
          left_late, right_late, window, spread):
    me = lax.axis_index("tm")
    spot = lax.axis_index("rep")
    column = spot // PLANES
    plane = spot % PLANES
    bin_count = bins_ref.shape[0]
    snap_rows, elem_rows, samples = snaps.shape
    grid_rows = reps.shape[2]
    elems = reps.shape[3]

    def rep_at(col, z):
        return col * PLANES + lax.rem(z + 2 * PLANES, PLANES)

    assert max(max(UP), max(DOWN)) <= 6
    near = (-2, 2, -1, 1)

    def plane_at(offset):
        return lax.rem(plane + offset + PLANES, PLANES)

    bins_load = pltpu.make_async_copy(bins_hbm, bins_ref, load_sem.at[3])
    bins_load.start()
    snap_load = pltpu.make_async_copy(snaps_hbm, snaps, load_sem.at[0])
    snap_load.start()
    rep_loads = [pltpu.make_async_copy(reps_hbm.at[:, b], reps.at[:, b], load_sem.at[1 + b]) for b in range(2)]
    for load in rep_loads:
        load.start()


    barrier = pltpu.get_barrier_semaphore()

    pl.semaphore_signal(barrier, inc=1, device_id={"tm": me, "rep": rep_at(1 - column, plane)}, device_id_type=MESH)
    for d in near:
        pl.semaphore_signal(barrier, inc=1, device_id={"tm": me, "rep": rep_at(column, plane + d)},
                            device_id_type=MESH)

    def greet(off, carry):
        other = lax.rem(me + off, peers)
        pl.semaphore_signal(barrier, inc=1, device_id={"tm": other, "rep": rep_at(column, plane)}, device_id_type=MESH)
        return carry

    lax.fori_loop(1, peers, greet, 0)
    greeted = peers + len(near)

    lane = lane_iota((1, 128))
    unit = 2.0 * math.pi / samples
    window[...] = 0.5 - 0.5 * jnp.cos(lane_iota((1, samples)).astype(F32) * unit)
    wide = lane_iota((1, 4 * 128))
    quarter = me % 4
    owner = (wide // 128) * 4 + (((wide // 32) % 4 + 4 - quarter) & 3)
    key = owner * 4 + (wide // 8) % 4
    spread[...] = (lax.broadcasted_iota(jnp.int32, (128, 512), 0) & 63 == key).astype(F32).astype(BF16)

    for k in range(4):
        blocks[1, plane_at(LATE + k)] = jnp.zeros((4, 8, 128), F32)
    right_late[:, 192:, :] = jnp.zeros((2, 64, 256), BF16)
    bins_load.wait()
    chosen = jnp.zeros((1, 128), jnp.int32)
    for k in range(bin_count):
        chosen = jnp.where((lane & 63) // 2 == k, bins_ref[k], chosen)
    index = lax.broadcasted_iota(jnp.int32, (32, 128), 0)
    coarse = ((index * 32 * chosen) & (samples - 1)).astype(F32) * unit
    fine = ((index * chosen) & (samples - 1)).astype(F32) * unit
    cos_a, sin_a = jnp.cos(coarse), jnp.sin(coarse)
    cos_b, sin_b = jnp.cos(fine), jnp.sin(fine)
    real = (lane & 1) == 0
    with_cos = jnp.where(real, cos_b, -sin_b)
    with_sin = jnp.where(real, -sin_b, -cos_b)
    for a in range(samples // 32):
        rows = cos_a[a : a + 1] * with_cos + sin_a[a : a + 1] * with_sin
        high = rows.astype(BF16).astype(F32)
        table[32 * a : 32 * a + 32, :] = jnp.where(lane < 64, high, rows - high).astype(BF16)

    snap_load.wait()
    shaded = snaps[...].reshape(snap_rows * elem_rows, samples) * window[...]
    high, low = split(shaded)
    spectra = jnp.dot(jnp.concatenate([high, low], axis=0), table[...], preferred_element_type=F32)
    high, low = split(spectra)
    placed = jnp.dot(jnp.concatenate([high, low], axis=0), spread[...], preferred_element_type=F32)
    slabs = jnp.sum(placed.reshape(4, snap_rows, elem_rows, 512), axis=0)
    merged = jnp.zeros((elem_rows, 512), F32)
    for s in range(snap_rows):
        merged = jnp.where((wide & 7) == s, slabs[s], merged)
    for tile in range(4):
        part = merged[:, 128 * tile : 128 * tile + 128]
        for d in range(4):
            pieces[4 * tile + d] = part if d == 0 else pltpu.roll(part, 128 - 32 * d, 1)
    landed[me] = pieces[me]

    pl.semaphore_wait(barrier, greeted)

    def report(sem):
        for d in (-2, 2):
            pl.semaphore_signal(sem, inc=1, device_id={"tm": me, "rep": rep_at(column, plane + d)},
                                device_id_type=MESH)

    report(ready.at[0])
    pl.semaphore_signal(ready.at[0], inc=1, device_id={"tm": me, "rep": rep_at(1 - column, plane)}, device_id_type=MESH)

    def piece_copy(other, source):
        return pltpu.make_async_remote_copy(
            src_ref=pieces.at[other], dst_ref=landed.at[source], send_sem=piece_send,
            recv_sem=piece_recv, device_id={"tm": other, "rep": rep_at(column, plane)}, device_id_type=MESH)

    def send_piece(off, carry):
        piece_copy(lax.rem(me + 1 + lax.rem(off + 10, peers - 1), peers), me).start()
        return carry

    lax.fori_loop(1, peers, send_piece, 0)

    near_lanes = pl.ds(pl.multiple_of(128 * column, 128), 128)
    far_lanes = pl.ds(pl.multiple_of(128 * (1 - column), 128), 128)
    turn = (8 * (2 * PLANES - LATE - plane)) & 127
    turn_im = (turn + 32) & 127
    def prepare_bin(b):
        rep_loads[b].wait()

        def prepare(step, carry, b=b):
            at = pl.ds(pl.multiple_of(step * 128, 128), 128)
            energy = jnp.zeros((128, 128), F32)
            parts = []
            for half, lanes in ((0, near_lanes), (1, far_lanes)):
                for part in range(2):
                    value = reps[part, b, at, lanes]
                    high, low = split(value)
                    to = 256 * half + 128 * part
                    left_hi[b, at, to : to + 128] = high
                    left_lo[b, at, to : to + 128] = low
                    energy = energy + value * value
                    parts.append(value)
            last = jnp.where(lane < 32, pltpu.roll(parts[2], turn, 1), pltpu.roll(parts[3], turn_im, 1))
            last = jnp.where(lane < 64, last, pltpu.roll(last, 64, 1))
            high, low = split(last)
            left_late[b, at, 0:128] = high
            left_late[b, at, 128:256] = low
            norms[b, pl.ds(step, 1), :] = row_sums(energy)
            return carry

        lax.fori_loop(0, grid_rows // 128, prepare, 0)

    prepare_bin(0)

    pl.semaphore_wait(ready.at[0], 3)
    report(ready.at[1])
    all_pieces = pltpu.make_async_remote_copy(
        src_ref=pieces.at[pl.ds(0, peers - 1)], dst_ref=landed.at[pl.ds(0, peers - 1)], send_sem=piece_send,
        recv_sem=piece_recv, device_id={"tm": lax.rem(me + 1, peers), "rep": spot}, device_id_type=MESH)
    all_pieces.wait_recv()

    tiles = []
    for tile in range(4):
        got = landed[4 * tile]
        for d in range(1, 4):
            got = jnp.where(lane // 32 == d, landed[4 * tile + d], got)
        tiles.append(got)
    for pair in range(2):
        first, second = tiles[2 * pair], tiles[2 * pair + 1]
        blocks[0, plane, pair] = jnp.where(lane & 16 == 0, first, pltpu.roll(second, 16, 1))
        blocks[0, plane, 2 + pair] = jnp.where(lane & 16 == 0, pltpu.roll(first, 112, 1), second)

    def block_copy(offset, to):
        owner_plane = plane_at(offset)
        return pltpu.make_async_remote_copy(
            src_ref=blocks.at[0, owner_plane], dst_ref=blocks.at[0, owner_plane], send_sem=block_send,
            recv_sem=block_recv.at[owner_plane], device_id={"tm": me, "rep": rep_at(column, plane + to)},
            device_id_type=MESH)

    late_count = late.shape[0]

    def cross(offset, to=0):
        owner_plane = plane_at(offset)
        slot = (offset - to - LATE) % PLANES
        target, sem = (late.at[slot], late_recv) if slot < late_count else (blocks.at[1, owner_plane], cross_recv)
        pltpu.make_async_remote_copy(
            src_ref=blocks.at[0, owner_plane], dst_ref=target, send_sem=cross_send, recv_sem=sem,
            device_id={"tm": me, "rep": rep_at(1 - column, plane + to)}, device_id_type=MESH).start()
        crossed.append((offset, to))

    crossed = []
    sent = []

    def pass_on(offset, to):
        block_copy(offset, to).start()
        sent.append((offset, to))

    def take(offset):
        block_copy(offset, 1).wait_recv()

    turned_sign = (lane & 8) == 0
    energies = [jnp.zeros((8, 128), F32) for _ in range(2)]

    def halves_of(value, b):
        turned = jnp.where(turned_sign, pltpu.roll(value, 120, 1), -pltpu.roll(value, 8, 1))
        energies[b] = energies[b] + jnp.sum((value * value).reshape(-1, 8, 128), axis=0)
        return split(value) + split(turned)

    def build(half):
        for b in range(2):
            for pair in range(2):
                to = slice(128 * pair, 128 * pair + 128)
                high, low, turned_high, turned_low = halves_of(
                    blocks[half, :, 2 * b + pair].reshape(PLANES * elem_rows, 128), b)
                at = 256 * half
                right_hi[b, at : at + 128, to] = high
                right_lo[b, at : at + 128, to] = low
                right_hi[b, at + 128 : at + 256, to] = turned_high
                right_lo[b, at + 128 : at + 256, to] = turned_low

    def build_late():
        for b in range(2):
            for pair in range(2):
                to = slice(128 * pair, 128 * pair + 128)
                high, low, turned_high, turned_low = halves_of(
                    late[:, 2 * b + pair].reshape(late_count * elem_rows, 128), b)
                for at, entry in enumerate((high, turned_high, low, turned_low, high, turned_high)):
                    right_late[b, 32 * at : 32 * at + 32, to] = entry

    def product(b, at, half):
        k = slice(256 * half, 256 * half + 256)
        value = jnp.dot(left_hi[b, at, k], right_hi[b, k, :], preferred_element_type=F32)
        value += jnp.dot(left_hi[b, at, k], right_lo[b, k, :], preferred_element_type=F32)
        return value + jnp.dot(left_lo[b, at, k], right_hi[b, k, :], preferred_element_type=F32)

    cross(0)

    pl.semaphore_wait(ready.at[1], 2)
    for hub in sorted(UP, reverse=True):
        pass_on(0, hub)
    for hub in sorted(DOWN, reverse=True):
        pass_on(0, -hub)
    prepare_bin(1)
    hubs = sorted([(hub, -hub, 1, leaves) for hub, leaves in UP.items()]
                  + [(hub, hub, -1, leaves) for hub, leaves in DOWN.items()])
    rest = []
    for hub, offset, way, leaves in hubs:
        take(offset)
        for leaf in leaves:
            pass_on(offset, way * leaf)
        if hub > 0:
            for leaf in leaves:
                cross(offset, way * leaf)
        cross(offset)
        rest += [(hub + leaf, -way * (hub + leaf), hub > 0) for leaf in leaves]
    for _, offset, done in sorted(rest):
        take(offset)
        if not done:
            cross(offset)
    assert len(crossed) == PLANES
    assert len(rest) + len(hubs) == PLANES - 1
    build(0)

    def project_near(step, carry):
        at = pl.ds(pl.multiple_of(step * ROWS, ROWS), ROWS)
        for b in range(2):
            halves[b, at, :] = product(b, at, 0)
        return carry

    lax.fori_loop(0, grid_rows // ROWS, project_near, 0)
    all_crossed = pltpu.make_async_remote_copy(
        src_ref=blocks.at[0], dst_ref=blocks.at[1], send_sem=cross_send, recv_sem=cross_recv,
        device_id={"tm": me, "rep": rep_at(1 - column, plane)}, device_id_type=MESH)
    early_crossed = pltpu.make_async_remote_copy(
        src_ref=blocks.at[0, pl.ds(0, PLANES - late_count)], dst_ref=blocks.at[1, pl.ds(0, PLANES - late_count)],
        send_sem=cross_send, recv_sem=cross_recv, device_id={"tm": me, "rep": rep_at(1 - column, plane)},
        device_id_type=MESH)
    late_crossed = pltpu.make_async_remote_copy(
        src_ref=late, dst_ref=late, send_sem=cross_send, recv_sem=late_recv,
        device_id={"tm": me, "rep": rep_at(1 - column, plane)}, device_id_type=MESH)
    early_crossed.wait_recv()
    build(1)

    def project_far(step, carry):
        at = pl.ds(pl.multiple_of(step * ROWS, ROWS), ROWS)
        for b in range(2):
            halves[b, at, :] += product(b, at, 1)
        return carry

    lax.fori_loop(0, grid_rows // ROWS, project_far, 0)
    late_crossed.wait_recv()
    build_late()

    def project(step, carry):
        at = pl.ds(pl.multiple_of(step * ROWS, ROWS), ROWS)
        for b in range(2):
            proj = halves[b, at, :] + jnp.dot(left_late[b, at, :], right_late[b], preferred_element_type=F32)
            square = proj * proj
            square = square[:, :128] + square[:, 128:]
            for piece in range(ROWS // 128):
                quads[b, pl.ds(step * (ROWS // 128) + piece, 1), :] = row_sums(square[128 * piece : 128 * piece + 128])
        return carry

    lax.fori_loop(0, grid_rows // ROWS, project, 0)
    traces = [jnp.sum(energy) for energy in energies]

    snap_total = snap_rows * peers
    power = jnp.zeros((grid_rows // 128, 128), F32)
    for b in range(2):
        trace = traces[b] / snap_total + EPS
        power = power + quads[b] / snap_total / ((norms[b] + EPS) * trace / elems)
    power = power / bin_count
    for r in range(grid_rows // 128):
        shares[r] = power[r : r + 1]
    arrived[me] = shares[me // 2]

    def send_share(off, carry):
        other = lax.rem(me + 1 + lax.rem(off + 10, peers - 1), peers)
        pltpu.make_async_remote_copy(
            src_ref=shares.at[other // 2], dst_ref=arrived.at[me], send_sem=share_send, recv_sem=share_recv,
            device_id={"tm": other, "rep": spot}, device_id_type=MESH).start()
        return carry

    lax.fori_loop(1, peers, send_share, 0)
    all_pieces.wait_send()
    all_crossed.wait_send()
    pltpu.make_async_remote_copy(
        src_ref=blocks.at[0, pl.ds(0, PLANES - 1)], dst_ref=blocks.at[0, pl.ds(0, PLANES - 1)], send_sem=block_send,
        recv_sem=block_recv.at[plane], device_id={"tm": me, "rep": rep_at(column, plane + 1)},
        device_id_type=MESH).wait_send()
    assert len(sent) == PLANES - 1
    all_shares = pltpu.make_async_remote_copy(
        src_ref=arrived.at[pl.ds(0, peers - 1)], dst_ref=arrived.at[pl.ds(0, peers - 1)], send_sem=share_send,
        recv_sem=share_recv, device_id={"tm": lax.rem(me + 1, peers), "rep": spot}, device_id_type=MESH)
    all_shares.wait_send()
    all_shares.wait_recv()
    total = jnp.sum(arrived[...], axis=0)
    odd = (me & 1) == 1
    out_ref[...] = jnp.where(odd, total[:, 64:], total[:, :64])


def shards(peers, snapshots, freq_bins, replicas):
    snap_rows, elem_rows, samples = snapshots.shape
    bins, grid_rows, elems = replicas.shape[1:]
    any_space = pl.BlockSpec(memory_space=pltpu.HBM)
    out = pl.pallas_call(
        functools.partial(fused, peers),
        out_shape=pltpu.VMEM((1, grid_rows // peers), F32),
        in_specs=[any_space, any_space, any_space],
        out_specs=pl.BlockSpec(memory_space=pltpu.VMEM),
        scratch_shapes=[
            pltpu.SMEM(freq_bins.shape, jnp.int32),
            pltpu.VMEM(snapshots.shape, F32),
            pltpu.VMEM(replicas.shape, F32),
            pltpu.VMEM((samples, 128), BF16),
            pltpu.VMEM((peers, 8, 128), F32),
            pltpu.VMEM((peers, 8, 128), F32),
            pltpu.VMEM((COLUMNS, PLANES, 4, 8, 128), F32),
            pltpu.VMEM((bins, grid_rows, 2 * elems), BF16),
            pltpu.VMEM((bins, grid_rows, 2 * elems), BF16),
            pltpu.VMEM((bins, grid_rows, 256), F32),
            pltpu.VMEM((bins, 2 * elems, 256), BF16),
            pltpu.VMEM((bins, 2 * elems, 256), BF16),
            pltpu.VMEM((bins, grid_rows // 128, 128), F32),
            pltpu.VMEM((bins, grid_rows // 128, 128), F32),
            pltpu.VMEM((grid_rows // 128, 1, 128), F32),
            pltpu.VMEM((peers, 1, 128), F32),
            pltpu.SemaphoreType.DMA((4,)),
            pltpu.SemaphoreType.DMA,
            pltpu.SemaphoreType.DMA,
            pltpu.SemaphoreType.DMA,
            pltpu.SemaphoreType.DMA((PLANES,)),
            pltpu.SemaphoreType.DMA,
            pltpu.SemaphoreType.DMA,
            pltpu.SemaphoreType.REGULAR((2,)),
            pltpu.SemaphoreType.DMA,
            pltpu.SemaphoreType.DMA,
            pltpu.SemaphoreType.DMA,
            pltpu.VMEM((4, 4, 8, 128), F32),
            pltpu.VMEM((bins, grid_rows, 256), BF16),
            pltpu.VMEM((bins, 256, 256), BF16),
            pltpu.VMEM((1, samples), F32),
            pltpu.VMEM((128, 512), BF16),
        ],
        compiler_params=pltpu.CompilerParams(collective_id=0, has_side_effects=True, vmem_limit_bytes=60 << 20),
    )(freq_bins, snapshots, replicas)
    return out.reshape(-1)


def solution(mesh):
    in_specs = (P("tm", "rep", None), P(), P(None, "tm", "rep", None))
    out_specs = P(("rep", "tm"))
    body = functools.partial(shards, mesh.shape["tm"])
    return jax.shard_map(body, mesh=mesh, in_specs=in_specs, out_specs=out_specs, check_vma=False)
```

```python
import functools
import math

import jax
import jax.numpy as jnp
from jax import lax
from jax.experimental import pallas as pl
from jax.experimental.pallas import tpu as pltpu
from jax.sharding import PartitionSpec as P

EPS = 1e-6
PLANES = 16
COLUMNS = 2
UP = {6: (2, 1, -1), 2: (2, 1, -1)}
DOWN = {5: (2, 1, -1), 2: (1, -1)}
LATE = 6
ROWS = 1024
MESH = pl.DeviceIdType.MESH
F32 = jnp.float32
BF16 = jnp.bfloat16


def split(value):
    high = value.astype(BF16)
    low = (value - high.astype(F32)).astype(BF16)
    return high, low


def lane_iota(shape):
    return lax.broadcasted_iota(jnp.int32, shape, len(shape) - 1)


def row_sums(value):
    return jnp.sum(value.T, axis=0, keepdims=True)


def fused(peers, bins_hbm, snaps_hbm, reps_hbm, out_ref, bins_ref, snaps, reps, table, pieces, landed, blocks, left_hi, left_lo, halves, right_hi,
          right_lo, norms, quads, shares, arrived, load_sem, piece_send, piece_recv, block_send, block_recv, share_send,
          share_recv, ready, cross_send, cross_recv, late_recv, late,
          left_late, right_late, window, spread):
    me = lax.axis_index("tm")
    spot = lax.axis_index("rep")
    column = spot // PLANES
    plane = spot % PLANES
    bin_count = bins_ref.shape[0]
    snap_rows, elem_rows, samples = snaps.shape
    grid_rows = reps.shape[2]
    elems = reps.shape[3]

    def rep_at(col, z):
        return col * PLANES + lax.rem(z + 2 * PLANES, PLANES)

    assert max(max(UP), max(DOWN)) <= 6
    near = (-2, 2, -1, 1)

    def plane_at(offset):
        return lax.rem(plane + offset + PLANES, PLANES)

    bins_load = pltpu.make_async_copy(bins_hbm, bins_ref, load_sem.at[3])
    bins_load.start()
    snap_load = pltpu.make_async_copy(snaps_hbm, snaps, load_sem.at[0])
    snap_load.start()
    rep_loads = [pltpu.make_async_copy(reps_hbm.at[:, b], reps.at[:, b], load_sem.at[1 + b]) for b in range(2)]
    for load in rep_loads:
        load.start()


    barrier = pltpu.get_barrier_semaphore()

    @pl.when(column == 0)
    def _():
        pl.semaphore_signal(barrier, inc=1, device_id={"tm": me, "rep": rep_at(1 - column, plane)},
                            device_id_type=MESH)

    for d in near:
        pl.semaphore_signal(barrier, inc=1, device_id={"tm": me, "rep": rep_at(column, plane + d)},
                            device_id_type=MESH)

    def greet(off, carry):
        other = lax.rem(me + off, peers)
        pl.semaphore_signal(barrier, inc=1, device_id={"tm": other, "rep": rep_at(column, plane)}, device_id_type=MESH)
        return carry

    lax.fori_loop(1, peers, greet, 0)
    greeted = peers - 1 + len(near) + column

    lane = lane_iota((1, 128))
    unit = 2.0 * math.pi / samples
    window[...] = 0.5 - 0.5 * jnp.cos(lane_iota((1, samples)).astype(F32) * unit)
    wide = lane_iota((1, 4 * 128))
    quarter = me % 4
    owner = (wide // 128) * 4 + (((wide // 32) % 4 + 4 - quarter) & 3)
    key = owner * 4 + (wide // 8) % 4
    spread[...] = (lax.broadcasted_iota(jnp.int32, (128, 512), 0) & 63 == key).astype(F32).astype(BF16)

    for k in range(4):
        blocks[1, plane_at(LATE + k)] = jnp.zeros((4, 8, 128), F32)
    right_late[:, 192:, :] = jnp.zeros((2, 64, 256), BF16)
    bins_load.wait()
    chosen = jnp.zeros((1, 128), jnp.int32)
    for k in range(bin_count):
        chosen = jnp.where((lane & 63) // 2 == k, bins_ref[k], chosen)
    index = lax.broadcasted_iota(jnp.int32, (32, 128), 0)
    coarse = ((index * 32 * chosen) & (samples - 1)).astype(F32) * unit
    fine = ((index * chosen) & (samples - 1)).astype(F32) * unit
    cos_a, sin_a = jnp.cos(coarse), jnp.sin(coarse)
    cos_b, sin_b = jnp.cos(fine), jnp.sin(fine)
    real = (lane & 1) == 0
    with_cos = jnp.where(real, cos_b, -sin_b)
    with_sin = jnp.where(real, -sin_b, -cos_b)
    for a in range(samples // 32):
        rows = cos_a[a : a + 1] * with_cos + sin_a[a : a + 1] * with_sin
        high = rows.astype(BF16).astype(F32)
        table[32 * a : 32 * a + 32, :] = jnp.where(lane < 64, high, rows - high).astype(BF16)

    snap_load.wait()
    shaded = snaps[...].reshape(snap_rows * elem_rows, samples) * window[...]
    high, low = split(shaded)
    spectra = jnp.dot(jnp.concatenate([high, low], axis=0), table[...], preferred_element_type=F32)
    high, low = split(spectra)
    placed = jnp.dot(jnp.concatenate([high, low], axis=0), spread[...], preferred_element_type=F32)
    slabs = jnp.sum(placed.reshape(4, snap_rows, elem_rows, 512), axis=0)
    merged = jnp.zeros((elem_rows, 512), F32)
    for s in range(snap_rows):
        merged = jnp.where((wide & 7) == s, slabs[s], merged)
    for tile in range(4):
        part = merged[:, 128 * tile : 128 * tile + 128]
        for d in range(4):
            pieces[4 * tile + d] = part if d == 0 else pltpu.roll(part, 128 - 32 * d, 1)
    landed[me] = pieces[me]

    pl.semaphore_wait(barrier, greeted)

    def report(sem):
        for d in (-2, 2):
            pl.semaphore_signal(sem, inc=1, device_id={"tm": me, "rep": rep_at(column, plane + d)},
                                device_id_type=MESH)

    def report_across(sem):
        pl.semaphore_signal(sem, inc=1, device_id={"tm": me, "rep": rep_at(1 - column, plane)}, device_id_type=MESH)

    report(ready.at[0])

    @pl.when(column == 1)
    def _():
        report_across(ready.at[0])

    def piece_copy(other, source):
        return pltpu.make_async_remote_copy(
            src_ref=pieces.at[other], dst_ref=landed.at[source], send_sem=piece_send,
            recv_sem=piece_recv, device_id={"tm": other, "rep": rep_at(column, plane)}, device_id_type=MESH)

    def send_piece(off, carry):
        piece_copy(lax.rem(me + 1 + lax.rem(off + 10, peers - 1), peers), me).start()
        return carry

    lax.fori_loop(1, peers, send_piece, 0)

    near_lanes = pl.ds(pl.multiple_of(128 * column, 128), 128)
    far_lanes = pl.ds(pl.multiple_of(128 * (1 - column), 128), 128)
    turn = (8 * (2 * PLANES - LATE - plane)) & 127
    turn_im = (turn + 32) & 127
    def prepare_bin(b):
        rep_loads[b].wait()

        def prepare(step, carry, b=b):
            at = pl.ds(pl.multiple_of(step * 128, 128), 128)
            energy = jnp.zeros((128, 128), F32)
            parts = []
            for half, lanes in ((0, near_lanes), (1, far_lanes)):
                for part in range(2):
                    value = reps[part, b, at, lanes]
                    high, low = split(value)
                    to = 256 * half + 128 * part
                    left_hi[b, at, to : to + 128] = high
                    left_lo[b, at, to : to + 128] = low
                    energy = energy + value * value
                    parts.append(value)
            last = jnp.where(lane < 32, pltpu.roll(parts[2], turn, 1), pltpu.roll(parts[3], turn_im, 1))
            last = jnp.where(lane < 64, last, pltpu.roll(last, 64, 1))
            high, low = split(last)
            left_late[b, at, 0:128] = high
            left_late[b, at, 128:256] = low
            norms[b, pl.ds(step, 1), :] = row_sums(energy)
            return carry

        lax.fori_loop(0, grid_rows // 128, prepare, 0)

    prepare_bin(0)

    pl.semaphore_wait(ready.at[0], 3 - column)
    report(ready.at[1])

    @pl.when(column == 0)
    def _():
        report_across(ready.at[1])

    all_pieces = pltpu.make_async_remote_copy(
        src_ref=pieces.at[pl.ds(0, peers - 1)], dst_ref=landed.at[pl.ds(0, peers - 1)], send_sem=piece_send,
        recv_sem=piece_recv, device_id={"tm": lax.rem(me + 1, peers), "rep": spot}, device_id_type=MESH)
    all_pieces.wait_recv()

    tiles = []
    for tile in range(4):
        got = landed[4 * tile]
        for d in range(1, 4):
            got = jnp.where(lane // 32 == d, landed[4 * tile + d], got)
        tiles.append(got)
    for pair in range(2):
        first, second = tiles[2 * pair], tiles[2 * pair + 1]
        blocks[0, plane, pair] = jnp.where(lane & 16 == 0, first, pltpu.roll(second, 16, 1))
        blocks[0, plane, 2 + pair] = jnp.where(lane & 16 == 0, pltpu.roll(first, 112, 1), second)

    def block_copy(offset, to):
        owner_plane = plane_at(offset)
        return pltpu.make_async_remote_copy(
            src_ref=blocks.at[0, owner_plane], dst_ref=blocks.at[0, owner_plane], send_sem=block_send,
            recv_sem=block_recv.at[owner_plane], device_id={"tm": me, "rep": rep_at(column, plane + to)},
            device_id_type=MESH)

    late_count = late.shape[0]

    def cross(offset, to=0):
        owner_plane = plane_at(offset)
        slot = (offset - to - LATE) % PLANES
        target, sem = (late.at[slot], late_recv) if slot < late_count else (blocks.at[1, owner_plane], cross_recv)
        pltpu.make_async_remote_copy(
            src_ref=blocks.at[0, owner_plane], dst_ref=target, send_sem=cross_send, recv_sem=sem,
            device_id={"tm": me, "rep": rep_at(1 - column, plane + to)}, device_id_type=MESH).start()
        crossed.append((offset, to))

    crossed = []
    sent = []

    def pass_on(offset, to):
        block_copy(offset, to).start()
        sent.append((offset, to))

    def take(offset):
        block_copy(offset, 1).wait_recv()

    turned_sign = (lane & 8) == 0
    energies = [jnp.zeros((8, 128), F32) for _ in range(2)]

    def halves_of(value, b):
        turned = jnp.where(turned_sign, pltpu.roll(value, 120, 1), -pltpu.roll(value, 8, 1))
        energies[b] = energies[b] + jnp.sum((value * value).reshape(-1, 8, 128), axis=0)
        return split(value) + split(turned)

    def build(half):
        for b in range(2):
            for pair in range(2):
                to = slice(128 * pair, 128 * pair + 128)
                high, low, turned_high, turned_low = halves_of(
                    blocks[half, :, 2 * b + pair].reshape(PLANES * elem_rows, 128), b)
                at = 256 * half
                right_hi[b, at : at + 128, to] = high
                right_lo[b, at : at + 128, to] = low
                right_hi[b, at + 128 : at + 256, to] = turned_high
                right_lo[b, at + 128 : at + 256, to] = turned_low

    def build_late():
        for b in range(2):
            for pair in range(2):
                to = slice(128 * pair, 128 * pair + 128)
                high, low, turned_high, turned_low = halves_of(
                    late[:, 2 * b + pair].reshape(late_count * elem_rows, 128), b)
                for at, entry in enumerate((high, turned_high, low, turned_low, high, turned_high)):
                    right_late[b, 32 * at : 32 * at + 32, to] = entry

    def product(b, at, half):
        k = slice(256 * half, 256 * half + 256)
        value = jnp.dot(left_hi[b, at, k], right_hi[b, k, :], preferred_element_type=F32)
        value += jnp.dot(left_hi[b, at, k], right_lo[b, k, :], preferred_element_type=F32)
        return value + jnp.dot(left_lo[b, at, k], right_hi[b, k, :], preferred_element_type=F32)


    pl.semaphore_wait(ready.at[1], 2 + column)
    cross(0)
    for hub in sorted(UP, reverse=True):
        pass_on(0, hub)
    for hub in sorted(DOWN, reverse=True):
        pass_on(0, -hub)
    prepare_bin(1)
    hubs = sorted([(hub, -hub, 1, leaves) for hub, leaves in UP.items()]
                  + [(hub, hub, -1, leaves) for hub, leaves in DOWN.items()])
    rest = []
    for hub, offset, way, leaves in hubs:
        take(offset)
        for leaf in leaves:
            pass_on(offset, way * leaf)
        if hub > 0:
            for leaf in leaves:
                cross(offset, way * leaf)
        cross(offset)
        rest += [(hub + leaf, -way * (hub + leaf), hub > 0) for leaf in leaves]
    for _, offset, done in sorted(rest):
        take(offset)
        if not done:
            cross(offset)
    assert len(crossed) == PLANES
    assert len(rest) + len(hubs) == PLANES - 1
    build(0)

    def project_near(step, carry):
        at = pl.ds(pl.multiple_of(step * ROWS, ROWS), ROWS)
        for b in range(2):
            halves[b, at, :] = product(b, at, 0)
        return carry

    lax.fori_loop(0, grid_rows // ROWS, project_near, 0)
    all_crossed = pltpu.make_async_remote_copy(
        src_ref=blocks.at[0], dst_ref=blocks.at[1], send_sem=cross_send, recv_sem=cross_recv,
        device_id={"tm": me, "rep": rep_at(1 - column, plane)}, device_id_type=MESH)
    early_crossed = pltpu.make_async_remote_copy(
        src_ref=blocks.at[0, pl.ds(0, PLANES - late_count)], dst_ref=blocks.at[1, pl.ds(0, PLANES - late_count)],
        send_sem=cross_send, recv_sem=cross_recv, device_id={"tm": me, "rep": rep_at(1 - column, plane)},
        device_id_type=MESH)
    late_crossed = pltpu.make_async_remote_copy(
        src_ref=late, dst_ref=late, send_sem=cross_send, recv_sem=late_recv,
        device_id={"tm": me, "rep": rep_at(1 - column, plane)}, device_id_type=MESH)
    early_crossed.wait_recv()
    build(1)

    def project_far(step, carry):
        at = pl.ds(pl.multiple_of(step * ROWS, ROWS), ROWS)
        for b in range(2):
            halves[b, at, :] += product(b, at, 1)
        return carry

    lax.fori_loop(0, grid_rows // ROWS, project_far, 0)
    late_crossed.wait_recv()
    build_late()

    def project(step, carry):
        at = pl.ds(pl.multiple_of(step * ROWS, ROWS), ROWS)
        for b in range(2):
            proj = halves[b, at, :] + jnp.dot(left_late[b, at, :], right_late[b], preferred_element_type=F32)
            square = proj * proj
            square = square[:, :128] + square[:, 128:]
            for piece in range(ROWS // 128):
                quads[b, pl.ds(step * (ROWS // 128) + piece, 1), :] = row_sums(square[128 * piece : 128 * piece + 128])
        return carry

    lax.fori_loop(0, grid_rows // ROWS, project, 0)
    traces = [jnp.sum(energy) for energy in energies]

    snap_total = snap_rows * peers
    power = jnp.zeros((grid_rows // 128, 128), F32)
    for b in range(2):
        trace = traces[b] / snap_total + EPS
        power = power + quads[b] / snap_total / ((norms[b] + EPS) * trace / elems)
    power = power / bin_count
    for r in range(grid_rows // 128):
        shares[r] = power[r : r + 1]
    arrived[me] = shares[me // 2]

    def send_share(off, carry):
        other = lax.rem(me + 1 + lax.rem(off + 10, peers - 1), peers)
        pltpu.make_async_remote_copy(
            src_ref=shares.at[other // 2], dst_ref=arrived.at[me], send_sem=share_send, recv_sem=share_recv,
            device_id={"tm": other, "rep": spot}, device_id_type=MESH).start()
        return carry

    lax.fori_loop(1, peers, send_share, 0)
    all_pieces.wait_send()
    all_crossed.wait_send()
    pltpu.make_async_remote_copy(
        src_ref=blocks.at[0, pl.ds(0, PLANES - 1)], dst_ref=blocks.at[0, pl.ds(0, PLANES - 1)], send_sem=block_send,
        recv_sem=block_recv.at[plane], device_id={"tm": me, "rep": rep_at(column, plane + 1)},
        device_id_type=MESH).wait_send()
    assert len(sent) == PLANES - 1
    all_shares = pltpu.make_async_remote_copy(
        src_ref=arrived.at[pl.ds(0, peers - 1)], dst_ref=arrived.at[pl.ds(0, peers - 1)], send_sem=share_send,
        recv_sem=share_recv, device_id={"tm": lax.rem(me + 1, peers), "rep": spot}, device_id_type=MESH)
    all_shares.wait_send()
    all_shares.wait_recv()
    total = jnp.sum(arrived[...], axis=0)
    odd = (me & 1) == 1
    out_ref[...] = jnp.where(odd, total[:, 64:], total[:, :64])


def shards(peers, snapshots, freq_bins, replicas):
    snap_rows, elem_rows, samples = snapshots.shape
    bins, grid_rows, elems = replicas.shape[1:]
    any_space = pl.BlockSpec(memory_space=pltpu.HBM)
    out = pl.pallas_call(
        functools.partial(fused, peers),
        out_shape=pltpu.VMEM((1, grid_rows // peers), F32),
        in_specs=[any_space, any_space, any_space],
        out_specs=pl.BlockSpec(memory_space=pltpu.VMEM),
        scratch_shapes=[
            pltpu.SMEM(freq_bins.shape, jnp.int32),
            pltpu.VMEM(snapshots.shape, F32),
            pltpu.VMEM(replicas.shape, F32),
            pltpu.VMEM((samples, 128), BF16),
            pltpu.VMEM((peers, 8, 128), F32),
            pltpu.VMEM((peers, 8, 128), F32),
            pltpu.VMEM((COLUMNS, PLANES, 4, 8, 128), F32),
            pltpu.VMEM((bins, grid_rows, 2 * elems), BF16),
            pltpu.VMEM((bins, grid_rows, 2 * elems), BF16),
            pltpu.VMEM((bins, grid_rows, 256), F32),
            pltpu.VMEM((bins, 2 * elems, 256), BF16),
            pltpu.VMEM((bins, 2 * elems, 256), BF16),
            pltpu.VMEM((bins, grid_rows // 128, 128), F32),
            pltpu.VMEM((bins, grid_rows // 128, 128), F32),
            pltpu.VMEM((grid_rows // 128, 1, 128), F32),
            pltpu.VMEM((peers, 1, 128), F32),
            pltpu.SemaphoreType.DMA((4,)),
            pltpu.SemaphoreType.DMA,
            pltpu.SemaphoreType.DMA,
            pltpu.SemaphoreType.DMA,
            pltpu.SemaphoreType.DMA((PLANES,)),
            pltpu.SemaphoreType.DMA,
            pltpu.SemaphoreType.DMA,
            pltpu.SemaphoreType.REGULAR((2,)),
            pltpu.SemaphoreType.DMA,
            pltpu.SemaphoreType.DMA,
            pltpu.SemaphoreType.DMA,
            pltpu.VMEM((4, 4, 8, 128), F32),
            pltpu.VMEM((bins, grid_rows, 256), BF16),
            pltpu.VMEM((bins, 256, 256), BF16),
            pltpu.VMEM((1, samples), F32),
            pltpu.VMEM((128, 512), BF16),
        ],
        compiler_params=pltpu.CompilerParams(collective_id=0, has_side_effects=True, vmem_limit_bytes=60 << 20),
    )(freq_bins, snapshots, replicas)
    return out.reshape(-1)


def solution(mesh):
    in_specs = (P("tm", "rep", None), P(), P(None, "tm", "rep", None))
    out_specs = P(("rep", "tm"))
    body = functools.partial(shards, mesh.shape["tm"])
    return jax.shard_map(body, mesh=mesh, in_specs=in_specs, out_specs=out_specs, check_vma=False)
```
